128 devices in a mesh: seq: 32 (over y, z, core), head: 4 (over x).
Axes of the slice: x: 4, y: 4, z: 4, core: 2. Of those that a mesh axis runs over, the one named last changes fastest.
Arguments:
- queries: bfloat16 [16384, 4096], P('seq', 'head'), may hold values from -5 to 5
- keys: bfloat16 [16384, 1024], P('seq', 'head'), may hold values from -5 to 5
- values: bfloat16 [16384, 1024], P('seq', 'head'), may hold values from -5 to 5
- doc_lengths: int32 [64], replicated, may hold values from 1 to 2048, 16384 in all
- out_weight: bfloat16 [4096, 4096], P('head', 'seq'), may hold values from -0.1875 to 0.1875
Outputs:
- mixed: bfloat16 [16384, 4096], P('seq', 'head')
The draws below stay inside these ranges and needn't reach their ends.
Inputs may be any that keep to these rules, and one draw needn't show every extreme that they name: `doc_lengths`: the lengths sum to 16384, and one document is exactly 2048 tokens long.
All inputs are finite; a program needn't handle non-finite values.
Results may differ from the reference program's by a relative error of at most 0.012.
Values may be sent and summed in bfloat16 or wider, within the bound.
A program may use at most 128 MiB of HBM per device.

```python
import math
import jax
import jax.numpy as jnp
import numpy as np
from jax import lax

D = 4096
HQ = 32
KV = 8
DH = 128
TOK_DEV = 512
TOKENS = 16384
MOST = 2048
DOCS = 64


def draw_keys(key, part):
    base = jnp.clip(jax.random.normal(jax.random.fold_in(key, 1), (TOKENS, KV * DH), jnp.float32), -5.0, 5.0)
    return base.astype(jnp.bfloat16)


def draw_queries(key, part):
    base = jnp.clip(jax.random.normal(jax.random.fold_in(key, 2), (TOKENS, HQ * DH), jnp.float32), -5.0, 5.0)
    return base.astype(jnp.bfloat16)


def raised(array, key, source, target, parts, factor):
    def block_of(axis_at):
        return (jnp.arange(array.shape[axis_at]) // (array.shape[axis_at] // parts)).reshape((-1,) + (1,) * (array.ndim - 1 - axis_at))

    one_side = jax.random.permutation(key, parts)[block_of(target)]
    other_side = (block_of(target) + parts // 2) % parts
    return jnp.where((block_of(source) == one_side) | (block_of(source) == other_side), factor * array, array)


def steps_of(key, dims, cuts, low, high):
    gain, own = 1.0, jax.random.fold_in(key, 6)
    for axis_at, parts in cuts:
        heights = jnp.exp(jax.random.uniform(jax.random.fold_in(own, axis_at), (parts,), jnp.float32, low / len(cuts), high / len(cuts)))
        gain = gain * jnp.repeat(heights, dims[axis_at] // parts).reshape([-1 if axis == axis_at else 1 for axis in range(len(dims))])
    return gain


def length_profile(amount, total, most, slope):
    loads = [(1 << 20) // math.isqrt(grade ** slope) + 1 for grade in range(2, amount + 1)]
    rest, given = total - most - (amount - 1), [1] * (amount - 1)
    while rest > 0:
        free = [i for i in range(amount - 1) if given[i] < most]
        mass, left = sum([loads[i] for i in free]), rest
        for i in free:
            addition = min(most - given[i], max(1, left * loads[i] // mass), rest)
            given[i] = given[i] + addition
            rest = rest - addition
    return np.array([most] + given)


def uneven(stream_key, count, total, limit, slope):
    if count == 2:
        one = jax.random.randint(stream_key, (), max(1, total - limit), min(limit, total - 1) + 1)
        return jnp.stack([one, total - one])
    sizes = jnp.asarray(length_profile(count, total, limit, slope), jnp.int32)
    twos = (count - 1) // 2
    source_of, taker = sizes[1:1 + 2 * twos:2], sizes[2:2 + 2 * twos:2]
    margin = jnp.minimum(source_of - 1, limit - taker)
    passed = jax.random.randint(jax.random.fold_in(stream_key, 1), (twos,), 0, 1 << 20) % (margin + 1)
    sizes = sizes.at[1:1 + 2 * twos:2].set(source_of - passed).at[2:2 + 2 * twos:2].set(taker + passed)
    return sizes[jax.random.permutation(jax.random.fold_in(stream_key, 2), count)]


def normal_values(rng, dims, deviation, limit, split=(), kind=jnp.bfloat16):
    array = jax.random.normal(rng, dims, jnp.float32) * deviation
    if len(split) > 0:
        array = steps_of(rng, dims, split, -0.22, 0.18) * array
    return jnp.clip(array, min=-limit, max=limit).astype(kind)


def heavy_noise(stream_key, dims, width, bound, shards, heavy, held_as=jnp.bfloat16):
    entries = width * jax.random.normal(stream_key, dims, jnp.float32)
    if shards:
        entries = entries * steps_of(stream_key, dims, shards, -0.22, 0.18)
    return jnp.clip(raised(entries, jax.random.fold_in(stream_key, 3), *heavy), -bound, bound).astype(held_as)


def setup_inputs(seed: int = 0) -> dict:
    seeds = jax.random.split(jax.random.key(seed), 6)
    return {
        "queries": draw_queries(jax.random.fold_in(seeds[5], 71), 0),
        "keys": draw_keys(jax.random.fold_in(seeds[5], 71), 0),
        "values": normal_values(seeds[2], (TOKENS, KV * DH), 1.0, 5.0, ((0, 32), (1, 4))),
        "doc_lengths": uneven(seeds[3], DOCS, TOKENS, MOST, 2).astype(jnp.int32),
        "out_weight": heavy_noise(seeds[4], (HQ * DH, D), (HQ * DH) ** -0.5, 0.1875, ((0, 4), (1, 32)), (0, 1, 32, 2.75)),
    }


def doc_index(positions, starts):
    return jnp.sum((starts[None, :] <= positions[:, None]).astype(jnp.int32), axis=1) - 1


def reference(queries, keys, values, doc_lengths, out_weight):
    starts = (jnp.cumsum(doc_lengths) - doc_lengths).astype(jnp.int32)
    total_rows = queries.shape[0]
    group_size = HQ // KV
    window = MOST + TOK_DEV
    num_blocks = total_rows // TOK_DEV
    temper = DH ** -0.5

    def attend_block(flat_index):
        q_block = flat_index // KV
        kv_head = flat_index % KV
        q_first = (q_block * TOK_DEV).astype(jnp.int32)
        k_first = jnp.clip(q_first - MOST, 0, total_rows - window).astype(jnp.int32)
        q_rows = lax.dynamic_slice(queries, (q_first, (kv_head * group_size * DH).astype(jnp.int32)), (TOK_DEV, group_size * DH))
        q_rows = q_rows.astype(jnp.float32).reshape(TOK_DEV, group_size, DH)
        k_rows = lax.dynamic_slice(keys, (k_first, (kv_head * DH).astype(jnp.int32)), (window, DH)).astype(jnp.float32)
        v_rows = lax.dynamic_slice(values, (k_first, (kv_head * DH).astype(jnp.int32)), (window, DH)).astype(jnp.float32)
        scores = jnp.einsum("qgd,nd->gqn", q_rows, k_rows) * temper
        q_pos = q_first + jnp.arange(TOK_DEV, dtype=jnp.int32)
        k_pos = k_first + jnp.arange(window, dtype=jnp.int32)
        q_doc = doc_index(q_pos, starts)
        k_doc = doc_index(k_pos, starts)
        allowed = (k_doc[None, :] == q_doc[:, None]) & (k_pos[None, :] <= q_pos[:, None])
        scores = jnp.where(allowed[None], scores, jnp.float32(-1e30))
        row_max = jnp.max(scores, axis=-1, keepdims=True)
        probs = jnp.where(allowed[None], jnp.exp(scores - row_max), jnp.float32(0.0))
        row_sum = jnp.sum(probs, axis=-1)
        weights = probs.astype(jnp.bfloat16)
        result = jnp.einsum("gqn,nd->gqd", weights.astype(jnp.float32), v_rows) / row_sum[..., None]
        return jnp.transpose(result, (1, 0, 2)).reshape(TOK_DEV, group_size * DH).astype(jnp.bfloat16)

    blocks = lax.map(attend_block, jnp.arange(num_blocks * KV, dtype=jnp.int32))
    attn = blocks.reshape(num_blocks, KV, TOK_DEV, group_size * DH)
    attn = jnp.transpose(attn, (0, 2, 1, 3)).reshape(total_rows, HQ * DH)
    return jnp.dot(attn, out_weight, preferred_element_type=jnp.float32).astype(jnp.bfloat16)
```

```python
import jax
import jax.numpy as jnp
from jax import lax
from jax.experimental import pallas as pl
from jax.experimental.pallas import tpu as pltpu
from jax.sharding import PartitionSpec as P

DH = 128
TOK = 512
ROWS = 2560
FAR = 16384.0
LOG2E = 1.4426950408889634
C2 = LOG2E * DH ** -0.5
F32 = jnp.float32
BF16 = jnp.bfloat16
MESH = pl.DeviceIdType.MESH


class Sems:
    def __init__(self, send, recv):
        self.send, self.recv, self.names, self.pending = send, recv, {}, []

    def index(self, name):
        return self.names.setdefault(name, len(self.names))

    def remote(self, name, src, dst, dev):
        i = self.index(name)
        return pltpu.make_async_remote_copy(
            src_ref=src, dst_ref=dst, send_sem=self.send.at[i], recv_sem=self.recv.at[i],
            device_id=dev, device_id_type=MESH)

    def go(self, name, src, dst, dev):
        d = self.remote(name, src, dst, dev)
        d.start()
        self.pending.append(d)
        return d


def kernel(q_ref, k_ref, v_ref, w_ref, len_ref, out_ref,
           qd, qcode, kd, kcode, vd, vrelay, wbuf, abuf, mbuf, acc, oacc, lens,
           loc_sem, send_sem, recv_sem, xs_sem, xr_sem):
    mx = lax.axis_index("head")
    s = lax.axis_index("seq")
    y = s // 8
    z = (s // 2) % 4
    c = s % 2
    sm = Sems(send_sem, recv_sem)

    def dev(seq, head=None):
        return {"seq": seq, "head": mx if head is None else head}

    def at(yy, zz, cc):
        return yy * 8 + zz * 2 + cc

    sib = dev(s + 1 - 2 * c)
    nxt = dev((s + 2) % 32)
    prv = dev((s + 30) % 32)
    zp, zm = dev(at(y, (z + 1) % 4, c)), dev(at(y, (z + 3) % 4, c))
    yp, ym = dev(at((y + 1) % 4, z, c)), dev(at((y + 3) % 4, z, c))
    xp, xm = dev(s, (mx + 1) % 4), dev(s, (mx + 3) % 4)
    p = y * 4 + z
    fwd = dev(((y * 4 + (z + 1) % 4 + 2) % 16) * 2 + c)
    po = (p + 14) % 16
    bwd = dev(at(po // 4, (po + 3) % 4, c))
    swap = {"seq": at(mx, z, c), "head": y}
    off = mx != y
    f1, f2 = z + c * (y - z), y + c * (z - y)

    def along(first, step):
        d1, d2 = (step, 0) if first else (0, step)
        i1, i2 = (f1 + d1) % 4, (f2 + d2) % 4
        yy, zz = i2 + c * (i1 - i2), i1 + c * (i2 - i1)
        return dev(at(yy, zz, c))

    def wblock(d1, d2):
        i1, i2 = (f1 + d1) % 4, (f2 + d2) % 4
        yy, zz = i2 + c * (i1 - i2), i1 + c * (i2 - i1)
        return wbuf.at[c, yy, zz]

    loc = []

    def local(src, dst):
        d = pltpu.make_async_copy(src, dst, loc_sem.at[len(loc)])
        d.start()
        loc.append(d)
        return d

    own = pl.ds(2048, TOK)
    lk = [local(k_ref.at[:, pl.ds(j * DH, DH)], kd.at[j, own]) for j in range(2)]
    lv = [local(v_ref.at[:, pl.ds(j * DH, DH)], vd.at[j, own]) for j in range(2)]
    lq = [local(q_ref.at[:, pl.ds(h * DH, DH)], qd.at[h]) for h in range(8)]

    barrier = pltpu.get_barrier_semaphore()
    for peer in (sib, nxt, prv, zp, zm, yp, ym, xp, xm, fwd, bwd):
        pl.semaphore_signal(barrier, inc=1, device_id=peer, device_id_type=MESH)

    @pl.when(off)
    def _():
        pl.semaphore_signal(barrier, inc=1, device_id=swap, device_id_type=MESH)

    lens[...] = jnp.zeros_like(lens)
    lens[0:1, 0:64] = len_ref[...]
    row = lens[0:1, :].astype(F32)
    i0 = lax.broadcasted_iota(jnp.int32, (DH, DH), 0)
    i1 = lax.broadcasted_iota(jnp.int32, (DH, DH), 1)
    col = jnp.sum(jnp.where(i1 < i0, jnp.broadcast_to(row, (DH, DH)), 0.0), axis=1, keepdims=True)
    start = jnp.sum(jnp.where(i0 == i1, jnp.broadcast_to(col, (DH, DH)), 0.0), axis=0, keepdims=True)
    end = start + row
    first = s * TOK

    @pl.loop(0, ROWS // 256)
    def _(b):
        pos = (first - 2048 + b * 256 + lax.broadcasted_iota(jnp.int32, (256, DH), 0)).astype(F32)
        inside = (pos >= start) & (pos < end)
        kcode[pl.ds(pl.multiple_of(b * 256, 256), 256), :] = jnp.where(inside, 0.0, -FAR).astype(BF16)

    for b in range(2):
        pos = (first + b * 256 + lax.broadcasted_iota(jnp.int32, (256, DH), 0)).astype(F32)
        inside = (pos >= start) & (pos < end)
        qcode[pl.ds(b * 256, 256), :] = jnp.where(inside, 1.0, 0.0).astype(BF16)

    for d in lk + lv:
        d.wait()
    pl.semaphore_wait(barrier, 11 + off.astype(jnp.int32))

    def slot(buf, j, i):
        start_row = (4 - i) * TOK
        if not isinstance(i, int):
            start_row = pl.multiple_of(start_row, TOK)
        return buf.at[j, pl.ds(start_row, TOK)]

    def both(name, j, src, dst, to):
        sm.go(f"{name}k{j}", slot(kd, j, src), slot(kd, j, dst), to)
        sm.go(f"{name}v{j}", slot(vd, j, src), slot(vd, j, dst), to)

    def both_recv(name, j, dst):
        sm.remote(f"{name}k{j}", slot(kd, j, dst), slot(kd, j, dst), sib).wait_recv()
        sm.remote(f"{name}v{j}", slot(vd, j, dst), slot(vd, j, dst), sib).wait_recv()

    def side(name, j, src, dst, when):
        ds = [sm.remote(f"{name}k{j}", slot(kd, j, src), slot(kd, j, dst), sib),
              sm.remote(f"{name}v{j}", slot(vd, j, src), slot(vd, j, dst), sib)]

        @pl.when(when)
        def _():
            for d in ds:
                d.start()
        return ds

    def kv_near(j):
        sm.go(f"relay{j}", slot(vd, j, 0), vrelay.at[j], zm)
        both("near", j, 0, 2, nxt)
        side("d1", j, 0, 1, c == 0)

    def kv_mid(j):
        both_recv("near", j, 2)
        sm.go(f"fark{j}", slot(kd, j, 2), slot(kd, j, 4), nxt)
        sm.remote(f"relay{j}", vrelay.at[j], vrelay.at[j], sib).wait_recv()
        sm.go(f"farv{j}", vrelay.at[j], slot(vd, j, 4), fwd)
        side("d1", j, 2, 1, c == 1)
        side("d2", j, 2, 3, c == 0)

    def kv_last(j):
        sm.remote(f"fark{j}", slot(kd, j, 4), slot(kd, j, 4), sib).wait_recv()
        sm.remote(f"farv{j}", slot(vd, j, 4), slot(vd, j, 4), sib).wait_recv()
        side("d2", j, 4, 3, c == 1)

    ones = jnp.ones((256, DH), BF16)

    def tile(h, j, qc, lo, n, init, diag, last):
        rows = pl.ds(qc * 256, 256)
        qa = jnp.concatenate([qd[h, rows, :], qcode[rows, :]], axis=1)
        ka = jnp.concatenate([kd[j, pl.ds(lo, n), :], kcode[pl.ds(lo, n), :]], axis=1)
        sc = lax.dot_general(qa, ka, (((1,), (1,)), ((), ())), preferred_element_type=F32)
        if diag:
            r = lax.broadcasted_iota(jnp.int32, (256, n), 0)
            u = lax.broadcasted_iota(jnp.int32, (256, n), 1)
            sc = jnp.where(u <= r + qc * 256, sc, -FAR)
        top = jnp.max(sc, axis=1, keepdims=True)
        if init:
            new = jnp.broadcast_to(top, (256, DH))
        else:
            old = mbuf[h, rows, :]
            new = jnp.maximum(old, top)
        pr = jnp.exp2((sc - jnp.concatenate([new] * (n // DH), axis=1)) * C2).astype(BF16)
        va = jnp.concatenate(
            [vd[j, pl.ds(lo, n), :], jnp.concatenate([ones] * (n // 256), axis=0)], axis=1)
        o = jnp.dot(pr, va, preferred_element_type=F32)
        if not init:
            fade = jnp.exp2((old - new) * C2)
            o = o + acc[h, rows, :] * jnp.concatenate([fade, fade], axis=1)
        if last:
            abuf[mx, h, rows, :] = (o[:, :DH] / o[:, DH:]).astype(BF16)
        else:
            mbuf[h, rows, :] = new
            acc[h, rows, :] = o

    def sweep(j, step, after=None):
        @pl.loop(0, 4)
        def _(g):
            h = j * 4 + g
            for qc in range(2):
                if step == 0:
                    tile(h, j, qc, 2048, 256 + 256 * qc, True, True, False)
                elif step == 1:
                    tile(h, j, qc, 1024, 1024, False, False, False)
                else:
                    tile(h, j, qc, 256 * qc, 1024 - 256 * qc, False, False, True)
            if after is not None:
                after(h)

    def xcopy(kind, h, block, lo, n, to):
        ref = abuf.at[block, h, pl.ds(lo, n)]
        return pltpu.make_async_remote_copy(
            src_ref=ref, dst_ref=ref, send_sem=xs_sem.at[kind, h], recv_sem=xr_sem.at[kind, h],
            device_id=to, device_id_type=MESH)

    xl, xr, xo = (mx + 3) % 4, (mx + 1) % 4, (mx + 2) % 4

    def xsend(h):
        xcopy(0, h, mx, 0, TOK, xp).start()
        xcopy(1, h, mx, 0, TOK, xm).start()

    def xrelay(h):
        xcopy(0, h, xl, 0, TOK, xp).wait_recv()
        xcopy(2, h, xl, 0, 256, xp).start()
        xcopy(1, h, xr, 0, TOK, xm).wait_recv()
        xcopy(3, h, xr, 256, 256, xm).start()

    def xdone(h):
        xcopy(2, h, xo, 0, 256, xp).wait_recv()
        xcopy(3, h, xo, 256, 256, xm).wait_recv()

    wt = sm.remote("wt", w_ref, wbuf.at[c, y, z], swap)
    wt_dst = sm.remote("wt", wbuf.at[c, y, z], wbuf.at[c, y, z], swap)
    wl = pltpu.make_async_copy(w_ref, wbuf.at[c, y, z], loc_sem.at[12])

    def w_swap():
        @pl.when(off)
        def _():
            pltpu.make_async_remote_copy(
                src_ref=w_ref, dst_ref=wbuf.at[c, mx, z], send_sem=send_sem.at[sm.index("wt")],
                recv_sem=recv_sem.at[sm.index("wt")], device_id=swap, device_id_type=MESH).start()

        @pl.when(jnp.logical_not(off))
        def _():
            wl.start()

    def w_swapped():
        @pl.when(off)
        def _():
            wt_dst.wait_recv()

        @pl.when(jnp.logical_not(off))
        def _():
            wl.wait()

    def w_side(d1, d2):
        b = wblock(d1, d2)
        sm.go(f"ws{d1}{d2}", b, b, sib)

    def w_send(d1, d2, second):
        b = wblock(d1, d2)
        sm.go(f"w{second}+{d1}", b, b, along(not second, 1))
        sm.go(f"w{second}-{d1}", b, b, along(not second, -1))

    def w_relay(d1, second):
        a, b = ((d1, -1), (d1, 1)) if second else ((-1, 0), (1, 0))
        ra, rb = wblock(*a), wblock(*b)
        sm.remote(f"w{second}+{d1}", ra, ra, sib).wait_recv()
        h = ra.at[pl.ds(0, 512)]
        sm.go(f"wr{second}+{d1}", h, h, along(not second, 1))
        w_side(*a)
        sm.remote(f"w{second}-{d1}", rb, rb, sib).wait_recv()
        h = rb.at[pl.ds(512, 512)]
        sm.go(f"wr{second}-{d1}", h, h, along(not second, -1))
        w_side(*b)

    def w_far(d1, second):
        o = (d1, 2) if second else (2, 0)
        b = wblock(*o)
        sm.remote(f"wr{second}+{d1}", b.at[pl.ds(0, 512)], b.at[pl.ds(0, 512)], sib).wait_recv()
        sm.remote(f"wr{second}-{d1}", b.at[pl.ds(512, 512)], b.at[pl.ds(512, 512)], sib).wait_recv()
        w_side(*o)

    kv_near(0)
    w_swap()
    for d in lq:
        d.wait()
    sweep(0, 0)
    sweep(1, 0)
    kv_mid(0)
    kv_near(1)
    w_swapped()
    w_side(0, 0)
    w_send(0, 0, 0)
    w_send(0, 0, 1)
    both_recv("d1", 0, 1)
    sweep(0, 1)
    kv_last(0)
    both_recv("d2", 0, 3)
    sweep(0, 2, xsend)
    kv_mid(1)
    w_relay(0, 0)
    w_send(-1, 0, 1)
    w_send(1, 0, 1)
    both_recv("d1", 1, 1)
    sweep(1, 1)
    w_far(0, 0)
    w_send(2, 0, 1)
    w_relay(0, 1)
    xrelay(0)
    xrelay(1)
    kv_last(1)
    both_recv("d2", 1, 3)
    sweep(1, 2, xsend)

    xrelay(2)
    xrelay(3)
    w_far(0, 1)
    w_relay(-1, 1)
    w_relay(1, 1)
    xrelay(4)
    xrelay(5)
    w_far(-1, 1)
    w_far(1, 1)
    w_relay(2, 1)
    xrelay(6)
    xrelay(7)
    w_far(2, 1)
    ws_dst = [(d1, d2) for d1 in (0, -1, 1, 2) for d2 in (0, -1, 1, 2)]
    other = 1 - c
    for d1, d2 in ws_dst:
        sm.remote(f"ws{d1}{d2}", wbuf.at[other, 0, 0], wbuf.at[other, 0, 0], sib).wait_recv()

    def project(block, j, init, last=False):
        @pl.loop(0, 8)
        def _(t):
            cc, r = t // 4, pl.ds(pl.multiple_of((t % 4) * 128, 128), 128)
            a = jnp.concatenate([abuf[block, j * 4 + g, r, :] for g in range(4)], axis=1)
            w = jnp.concatenate([wbuf[cc, block, b, pl.ds(j * 512, 512), :] for b in range(4)], axis=1)
            o = jnp.dot(a, w, preferred_element_type=F32)
            if not init:
                o = o + oacc[cc, r, :]
            oacc[cc, r, :] = o

    project(mx, 0, True)
    project(mx, 1, False)
    for j in range(2):
        project(xl, j, False)
        project(xr, j, False)
    for h in range(8):
        xdone(h)
    for j in range(2):
        project(xo, j, False)
    for cc in range(2):
        for b in range(4):
            out_ref[:, (2 * b + cc) * 128:(2 * b + cc + 1) * 128] = oacc[cc, :, b * 128:(b + 1) * 128].astype(BF16)

    for d in sm.pending:
        d.wait_send()
    for j in range(2):
        for kv in "kv":
            buf = kd if kv == "k" else vd
            r = slot(buf, j, 0)
            sm.remote(f"d1{kv}{j}", r, r, sib).wait_send()
            sm.remote(f"d2{kv}{j}", r, r, sib).wait_send()

    @pl.when(off)
    def _():
        wt.wait_send()
    for h in range(8):
        xcopy(0, h, mx, 0, TOK, xp).wait_send()
        xcopy(1, h, mx, 0, TOK, xm).wait_send()
        xcopy(2, h, xl, 0, 256, xp).wait_send()
        xcopy(3, h, xr, 256, 256, xm).wait_send()


def body(queries, keys, values, doc_lengths, out_weight):
    hbm = pl.BlockSpec(memory_space=pl.ANY)
    vmem = pl.BlockSpec(memory_space=pltpu.VMEM)
    return pl.pallas_call(
        kernel,
        out_shape=jax.ShapeDtypeStruct((TOK, 1024), BF16),
        in_specs=[hbm, hbm, hbm, hbm, vmem],
        out_specs=vmem,
        scratch_shapes=[
            pltpu.VMEM((8, TOK, DH), BF16),
            pltpu.VMEM((TOK, DH), BF16),
            pltpu.VMEM((2, ROWS, DH), BF16),
            pltpu.VMEM((ROWS, DH), BF16),
            pltpu.VMEM((2, ROWS, DH), BF16),
            pltpu.VMEM((2, TOK, DH), BF16),
            pltpu.VMEM((2, 4, 4, 1024, DH), BF16),
            pltpu.VMEM((4, 8, TOK, DH), BF16),
            pltpu.VMEM((8, TOK, DH), F32),
            pltpu.VMEM((8, TOK, 2 * DH), F32),
            pltpu.VMEM((2, TOK, 512), F32),
            pltpu.VMEM((8, DH), jnp.int32),
            pltpu.SemaphoreType.DMA((13,)),
            pltpu.SemaphoreType.DMA((64,)),
            pltpu.SemaphoreType.DMA((64,)),
            pltpu.SemaphoreType.DMA((4, 8)),
            pltpu.SemaphoreType.DMA((4, 8)),
        ],
        compiler_params=pltpu.CompilerParams(
            collective_id=0, has_side_effects=True, vmem_limit_bytes=60 * 1024 * 1024),
        name="attention_block",
    )(queries, keys, values, out_weight, doc_lengths.reshape(1, 64))


def solution(mesh):
    return jax.shard_map(
        body,
        mesh=mesh,
        in_specs=(P("seq", "head"), P("seq", "head"), P("seq", "head"), P(), P("head", "seq")),
        out_specs=P("seq", "head"),
        check_vma=False,
    )
```

```python
import jax
import jax.numpy as jnp
from jax import lax
from jax.experimental import pallas as pl
from jax.experimental.pallas import tpu as pltpu
from jax.sharding import PartitionSpec as P

DH = 128
TOK = 512
ROWS = 2560
FAR = 16384.0
LOG2E = 1.4426950408889634
C2 = LOG2E * DH ** -0.5
F32 = jnp.float32
BF16 = jnp.bfloat16
MESH = pl.DeviceIdType.MESH


class Sems:
    def __init__(self, send, recv):
        self.send, self.recv, self.names, self.pending = send, recv, {}, []

    def index(self, name):
        return self.names.setdefault(name, len(self.names))

    def remote(self, name, src, dst, dev):
        i = self.index(name)
        return pltpu.make_async_remote_copy(
            src_ref=src, dst_ref=dst, send_sem=self.send.at[i], recv_sem=self.recv.at[i],
            device_id=dev, device_id_type=MESH)

    def go(self, name, src, dst, dev):
        d = self.remote(name, src, dst, dev)
        d.start()
        self.pending.append(d)
        return d


def kernel(q_ref, k_ref, v_ref, w_ref, len_ref, out_ref,
           qd, qcode, kd, kcode, vd, vrelay, wbuf, abuf, mbuf, acc, oacc, lens,
           loc_sem, send_sem, recv_sem, xs_sem, xr_sem):
    mx = lax.axis_index("head")
    s = lax.axis_index("seq")
    y = s // 8
    z = (s // 2) % 4
    c = s % 2
    sm = Sems(send_sem, recv_sem)

    def dev(seq, head=None):
        return {"seq": seq, "head": mx if head is None else head}

    def at(yy, zz, cc):
        return yy * 8 + zz * 2 + cc

    sib = dev(s + 1 - 2 * c)
    nxt = dev((s + 2) % 32)
    prv = dev((s + 30) % 32)
    zp, zm = dev(at(y, (z + 1) % 4, c)), dev(at(y, (z + 3) % 4, c))
    yp, ym = dev(at((y + 1) % 4, z, c)), dev(at((y + 3) % 4, z, c))
    xp, xm = dev(s, (mx + 1) % 4), dev(s, (mx + 3) % 4)
    p = y * 4 + z
    fwd = dev(((y * 4 + (z + 1) % 4 + 2) % 16) * 2 + c)
    po = (p + 14) % 16
    bwd = dev(at(po // 4, (po + 3) % 4, c))
    swap = {"seq": at(mx, z, c), "head": y}
    off = mx != y
    f1, f2 = z + c * (y - z), y + c * (z - y)

    def along(first, step):
        d1, d2 = (step, 0) if first else (0, step)
        i1, i2 = (f1 + d1) % 4, (f2 + d2) % 4
        yy, zz = i2 + c * (i1 - i2), i1 + c * (i2 - i1)
        return dev(at(yy, zz, c))

    def wblock(d1, d2):
        i1, i2 = (f1 + d1) % 4, (f2 + d2) % 4
        yy, zz = i2 + c * (i1 - i2), i1 + c * (i2 - i1)
        return wbuf.at[c, yy, zz]

    loc = []

    def local(src, dst):
        d = pltpu.make_async_copy(src, dst, loc_sem.at[len(loc)])
        d.start()
        loc.append(d)
        return d

    own = pl.ds(2048, TOK)
    lk = [local(k_ref.at[:, pl.ds(j * DH, DH)], kd.at[j, own]) for j in range(2)]
    lv = [local(v_ref.at[:, pl.ds(j * DH, DH)], vd.at[j, own]) for j in range(2)]
    lq = [local(q_ref.at[:, pl.ds(h * DH, DH)], qd.at[h]) for h in range(8)]

    barrier = pltpu.get_barrier_semaphore()
    for peer in (sib, nxt, prv, zp, zm, yp, ym, xp, xm, fwd, bwd):
        pl.semaphore_signal(barrier, inc=1, device_id=peer, device_id_type=MESH)

    @pl.when(off)
    def _():
        pl.semaphore_signal(barrier, inc=1, device_id=swap, device_id_type=MESH)

    lens[...] = jnp.zeros_like(lens)
    lens[0:1, 0:64] = len_ref[...]
    row = lens[0:1, :].astype(F32)
    i0 = lax.broadcasted_iota(jnp.int32, (DH, DH), 0)
    i1 = lax.broadcasted_iota(jnp.int32, (DH, DH), 1)
    col = jnp.sum(jnp.where(i1 < i0, jnp.broadcast_to(row, (DH, DH)), 0.0), axis=1, keepdims=True)
    start = jnp.sum(jnp.where(i0 == i1, jnp.broadcast_to(col, (DH, DH)), 0.0), axis=0, keepdims=True)
    end = start + row
    first = s * TOK

    @pl.loop(0, ROWS // 256)
    def _(b):
        pos = (first - 2048 + b * 256 + lax.broadcasted_iota(jnp.int32, (256, DH), 0)).astype(F32)
        inside = (pos >= start) & (pos < end)
        kcode[pl.ds(pl.multiple_of(b * 256, 256), 256), :] = jnp.where(inside, 0.0, -FAR).astype(BF16)

    for b in range(2):
        pos = (first + b * 256 + lax.broadcasted_iota(jnp.int32, (256, DH), 0)).astype(F32)
        inside = (pos >= start) & (pos < end)
        qcode[pl.ds(b * 256, 256), :] = jnp.where(inside, 1.0, 0.0).astype(BF16)

    for d in lk + lv:
        d.wait()
    pl.semaphore_wait(barrier, 11 + off.astype(jnp.int32))

    def slot(buf, j, i):
        start_row = (4 - i) * TOK
        if not isinstance(i, int):
            start_row = pl.multiple_of(start_row, TOK)
        return buf.at[j, pl.ds(start_row, TOK)]

    def both(name, j, src, dst, to):
        sm.go(f"{name}k{j}", slot(kd, j, src), slot(kd, j, dst), to)
        sm.go(f"{name}v{j}", slot(vd, j, src), slot(vd, j, dst), to)

    def both_recv(name, j, dst):
        sm.remote(f"{name}k{j}", slot(kd, j, dst), slot(kd, j, dst), sib).wait_recv()
        sm.remote(f"{name}v{j}", slot(vd, j, dst), slot(vd, j, dst), sib).wait_recv()

    def side(name, j, src, dst, when):
        ds = [sm.remote(f"{name}k{j}", slot(kd, j, src), slot(kd, j, dst), sib),
              sm.remote(f"{name}v{j}", slot(vd, j, src), slot(vd, j, dst), sib)]

        @pl.when(when)
        def _():
            for d in ds:
                d.start()
        return ds

    def kv_near(j):
        sm.go(f"relay{j}", slot(vd, j, 0), vrelay.at[j], zm)
        both("near", j, 0, 2, nxt)
        side("d1", j, 0, 1, c == 0)

    def kv_fwd(j):
        sm.remote(f"relay{j}", vrelay.at[j], vrelay.at[j], sib).wait_recv()
        sm.go(f"farv{j}", vrelay.at[j], slot(vd, j, 4), fwd)

    def kv_mid(j):
        sm.remote(f"neark{j}", slot(kd, j, 2), slot(kd, j, 2), sib).wait_recv()
        sm.go(f"fark{j}", slot(kd, j, 2), slot(kd, j, 4), nxt)

    def kv_side(j):
        sm.remote(f"nearv{j}", slot(vd, j, 2), slot(vd, j, 2), sib).wait_recv()
        side("d1", j, 2, 1, c == 1)
        side("d2", j, 2, 3, c == 0)

    def kv_last(j):
        sm.remote(f"fark{j}", slot(kd, j, 4), slot(kd, j, 4), sib).wait_recv()
        sm.remote(f"farv{j}", slot(vd, j, 4), slot(vd, j, 4), sib).wait_recv()
        side("d2", j, 4, 3, c == 1)

    ones = jnp.ones((256, DH), BF16)

    def tile(h, j, qc, lo, n, init, diag, last):
        rows = pl.ds(qc * 256, 256)
        qa = jnp.concatenate([qd[h, rows, :], qcode[rows, :]], axis=1)
        ka = jnp.concatenate([kd[j, pl.ds(lo, n), :], kcode[pl.ds(lo, n), :]], axis=1)
        sc = lax.dot_general(qa, ka, (((1,), (1,)), ((), ())), preferred_element_type=F32)
        if diag:
            r = lax.broadcasted_iota(jnp.int32, (256, n), 0)
            u = lax.broadcasted_iota(jnp.int32, (256, n), 1)
            sc = jnp.where(u <= r + qc * 256, sc, -FAR)
        top = jnp.max(sc, axis=1, keepdims=True)
        if init:
            new = jnp.broadcast_to(top, (256, DH))
        else:
            old = mbuf[h, rows, :]
            new = jnp.maximum(old, top)
        pr = jnp.exp2((sc - jnp.concatenate([new] * (n // DH), axis=1)) * C2).astype(BF16)
        va = jnp.concatenate(
            [vd[j, pl.ds(lo, n), :], jnp.concatenate([ones] * (n // 256), axis=0)], axis=1)
        o = jnp.dot(pr, va, preferred_element_type=F32)
        if not init:
            fade = jnp.exp2((old - new) * C2)
            o = o + acc[h, rows, :] * jnp.concatenate([fade, fade], axis=1)
        if last:
            abuf[mx, h, rows, :] = (o[:, :DH] / o[:, DH:]).astype(BF16)
        else:
            mbuf[h, rows, :] = new
            acc[h, rows, :] = o

    def sweep(j, step, after=None):
        @pl.loop(0, 4)
        def _(g):
            h = j * 4 + g
            for qc in range(2):
                if step == 0:
                    tile(h, j, qc, 2048, 256 + 256 * qc, True, True, False)
                elif step == 1:
                    tile(h, j, qc, 1024, 1024, False, False, False)
                else:
                    tile(h, j, qc, 256 * qc, 1024 - 256 * qc, False, False, True)
            if after is not None:
                after(h)

    def xcopy(kind, h, block, lo, n, to):
        ref = abuf.at[block, h, pl.ds(lo, n)]
        return pltpu.make_async_remote_copy(
            src_ref=ref, dst_ref=ref, send_sem=xs_sem.at[kind, h], recv_sem=xr_sem.at[kind, h],
            device_id=to, device_id_type=MESH)

    xl, xr, xo = (mx + 3) % 4, (mx + 1) % 4, (mx + 2) % 4

    def xsend(h):
        xcopy(0, h, mx, 0, TOK, xp).start()
        xcopy(1, h, mx, 0, TOK, xm).start()

    def xrelay(h):
        xcopy(0, h, xl, 0, TOK, xp).wait_recv()
        xcopy(2, h, xl, 0, 256, xp).start()
        xcopy(1, h, xr, 0, TOK, xm).wait_recv()
        xcopy(3, h, xr, 256, 256, xm).start()

    def xdone(h):
        xcopy(2, h, xo, 0, 256, xp).wait_recv()
        xcopy(3, h, xo, 256, 256, xm).wait_recv()

    def half(ref, i):
        return ref.at[pl.ds(512 * i, 512)]

    def wt(i, src, dst):
        return sm.remote(f"wt{i}", half(src, i), half(dst, i), swap)

    def wl(i):
        return pltpu.make_async_copy(half(w_ref, i), half(wbuf.at[c, y, z], i), loc_sem.at[12 + i])

    def w_swap():
        @pl.when(off)
        def _():
            for i in range(2):
                wt(i, w_ref, wbuf.at[c, mx, z]).start()

        @pl.when(jnp.logical_not(off))
        def _():
            for i in range(2):
                wl(i).start()

    def w_swapped(i):
        @pl.when(off)
        def _():
            wt(i, wbuf.at[c, y, z], wbuf.at[c, y, z]).wait_recv()

        @pl.when(jnp.logical_not(off))
        def _():
            wl(i).wait()

    def w_side(d1, d2):
        b = wblock(d1, d2)
        sm.go(f"ws{d1}{d2}", b, b, sib)

    def w_send(d1, d2, second, halves=(0, 1)):
        b = wblock(d1, d2)
        for i in halves:
            for sign, k in (("+", i), ("-", 1 - i if len(halves) == 2 else i)):
                sm.go(f"w{second}{sign}{d1}h{k}", half(b, k), half(b, k),
                      along(not second, 1 if sign == "+" else -1))

    def w_got(sign, d1, second, i, b):
        sm.remote(f"w{second}{sign}{d1}h{i}", half(b, i), half(b, i), sib).wait_recv()

    def w_pair(d1, second):
        a, b = ((d1, -1), (d1, 1)) if second else ((-1, 0), (1, 0))
        return a, b

    def w_relay(d1, second):
        a, b = w_pair(d1, second)
        ra, rb = wblock(*a), wblock(*b)
        w_got("+", d1, second, 0, ra)
        sm.go(f"wr{second}+{d1}", half(ra, 0), half(ra, 0), along(not second, 1))
        w_got("-", d1, second, 1, rb)
        sm.go(f"wr{second}-{d1}", half(rb, 1), half(rb, 1), along(not second, -1))

    def w_rest(d1, second):
        a, b = w_pair(d1, second)
        w_got("+", d1, second, 1, wblock(*a))
        w_side(*a)
        w_got("-", d1, second, 0, wblock(*b))
        w_side(*b)

    def w_far(d1, second):
        o = (d1, 2) if second else (2, 0)
        b = wblock(*o)
        sm.remote(f"wr{second}+{d1}", half(b, 0), half(b, 0), sib).wait_recv()
        sm.remote(f"wr{second}-{d1}", half(b, 1), half(b, 1), sib).wait_recv()
        w_side(*o)

    def project(block, js, init, last=False):
        @pl.loop(0, 4)
        def _(t):
            cc, b = t // 2, (t % 2) * 2
            hs = [j * 4 + g for j in js for g in range(4)]
            a = jnp.concatenate([abuf[block, h] for h in hs], axis=1)
            ks = pl.ds(js[0] * 512, 512 * len(js))
            w = jnp.concatenate([wbuf[cc, block, b, ks, :], wbuf[cc, block, b + 1, ks, :]], axis=1)
            o = jnp.dot(a, w, preferred_element_type=F32)
            if not init:
                o = o + oacc[t]
            if last:
                for i in range(2):
                    cols = pl.ds(pl.multiple_of((2 * (b + i) + cc) * 128, 128), 128)
                    out_ref[:, cols] = o[:, i * 128:(i + 1) * 128].astype(BF16)
            else:
                oacc[t] = o

    kv_near(0)
    w_swap()
    for d in lq:
        d.wait()
    sweep(0, 0)
    kv_fwd(0)
    sweep(1, 0)
    kv_mid(0)
    kv_near(1)
    kv_side(0)
    both_recv("d1", 0, 1)
    sweep(0, 1)
    kv_fwd(1)
    w_swapped(0)
    w_send(0, 0, 0, (0,))
    kv_last(0)
    both_recv("d2", 0, 3)
    sweep(0, 2, xsend)
    w_swapped(1)
    w_send(0, 0, 0, (1,))
    w_side(0, 0)
    kv_mid(1)
    kv_side(1)
    w_send(0, 0, 1)
    both_recv("d1", 1, 1)
    sweep(1, 1)
    w_relay(0, 0)
    w_rest(0, 0)
    w_send(-1, 0, 1)
    w_send(1, 0, 1)
    xrelay(0)
    kv_last(1)
    both_recv("d2", 1, 3)
    sweep(1, 2, xsend)
    w_far(0, 0)
    w_send(2, 0, 1)
    w_relay(0, 1)
    xrelay(1)
    w_rest(0, 1)
    xrelay(2)
    w_relay(-1, 1)
    w_relay(1, 1)
    xrelay(3)
    w_rest(-1, 1)
    w_rest(1, 1)
    w_far(0, 1)
    w_relay(2, 1)
    xrelay(4)
    w_rest(2, 1)
    w_far(-1, 1)
    w_far(1, 1)
    xrelay(5)
    w_far(2, 1)
    for d1 in (0, -1, 1, 2):
        for d2 in (0, -1, 1, 2):
            sm.remote(f"ws{d1}{d2}", wbuf.at[1 - c, 0, 0], wbuf.at[1 - c, 0, 0], sib).wait_recv()
    project(mx, (0, 1), True)
    xrelay(6)
    project(xl, (0,), False)
    project(xr, (0,), False)
    xrelay(7)
    for h in range(4):
        xdone(h)
    project(xo, (0,), False)
    project(xl, (1,), False)
    project(xr, (1,), False)
    for h in range(4, 8):
        xdone(h)
    project(xo, (1,), False, True)

    for d in sm.pending:
        d.wait_send()
    for j in range(2):
        for kv in "kv":
            buf = kd if kv == "k" else vd
            r = slot(buf, j, 0)
            sm.remote(f"d1{kv}{j}", r, r, sib).wait_send()
            sm.remote(f"d2{kv}{j}", r, r, sib).wait_send()

    @pl.when(off)
    def _():
        for i in range(2):
            wt(i, w_ref, wbuf.at[c, mx, z]).wait_send()
    for h in range(8):
        xcopy(0, h, mx, 0, TOK, xp).wait_send()
        xcopy(1, h, mx, 0, TOK, xm).wait_send()
        xcopy(2, h, xl, 0, 256, xp).wait_send()
        xcopy(3, h, xr, 256, 256, xm).wait_send()


def body(queries, keys, values, doc_lengths, out_weight):
    hbm = pl.BlockSpec(memory_space=pl.ANY)
    vmem = pl.BlockSpec(memory_space=pltpu.VMEM)
    return pl.pallas_call(
        kernel,
        out_shape=jax.ShapeDtypeStruct((TOK, 1024), BF16),
        in_specs=[hbm, hbm, hbm, hbm, vmem],
        out_specs=vmem,
        scratch_shapes=[
            pltpu.VMEM((8, TOK, DH), BF16),
            pltpu.VMEM((TOK, DH), BF16),
            pltpu.VMEM((2, ROWS, DH), BF16),
            pltpu.VMEM((ROWS, DH), BF16),
            pltpu.VMEM((2, ROWS, DH), BF16),
            pltpu.VMEM((2, TOK, DH), BF16),
            pltpu.VMEM((2, 4, 4, 1024, DH), BF16),
            pltpu.VMEM((4, 8, TOK, DH), BF16),
            pltpu.VMEM((8, TOK, DH), F32),
            pltpu.VMEM((8, TOK, 2 * DH), F32),
            pltpu.VMEM((4, TOK, 256), F32),
            pltpu.VMEM((8, DH), jnp.int32),
            pltpu.SemaphoreType.DMA((14,)),
            pltpu.SemaphoreType.DMA((96,)),
            pltpu.SemaphoreType.DMA((96,)),
            pltpu.SemaphoreType.DMA((4, 8)),
            pltpu.SemaphoreType.DMA((4, 8)),
        ],
        compiler_params=pltpu.CompilerParams(
            collective_id=0, has_side_effects=True, vmem_limit_bytes=60 * 1024 * 1024),
        name="attention_block",
    )(queries, keys, values, out_weight, doc_lengths.reshape(1, 64))


def solution(mesh):
    return jax.shard_map(
        body,
        mesh=mesh,
        in_specs=(P("seq", "head"), P("seq", "head"), P("seq", "head"), P(), P("head", "seq")),
        out_specs=P("seq", "head"),
        check_vma=False,
    )
```

```python
import jax
import jax.numpy as jnp
from jax import lax
from jax.experimental import pallas as pl
from jax.experimental.pallas import tpu as pltpu
from jax.sharding import PartitionSpec as P

DH = 128
TOK = 512
ROWS = 2560
FAR = 16384.0
LOG2E = 1.4426950408889634
C2 = LOG2E * DH ** -0.5
F32 = jnp.float32
BF16 = jnp.bfloat16
MESH = pl.DeviceIdType.MESH


class Sems:
    def __init__(self, send, recv):
        self.send, self.recv, self.names, self.pending = send, recv, {}, []

    def index(self, name):
        return self.names.setdefault(name, len(self.names))

    def remote(self, name, src, dst, dev):
        i = self.index(name)
        return pltpu.make_async_remote_copy(
            src_ref=src, dst_ref=dst, send_sem=self.send.at[i], recv_sem=self.recv.at[i],
            device_id=dev, device_id_type=MESH)

    def go(self, name, src, dst, dev):
        self.remote(name, src, dst, dev).start()
        self.pending.append((name, src.shape[0]))


def kernel(q_ref, k_ref, v_ref, w_ref, len_ref, out_ref,
           qd, qcode, kd, kcode, vd, vrelay, wrelay, wbuf, abuf, mbuf, acc, oacc, lens,
           loc_sem, send_sem, recv_sem, xs_sem, xr_sem):
    mx = lax.axis_index("head")
    s = lax.axis_index("seq")
    y = s // 8
    z = (s // 2) % 4
    c = s % 2
    sm = Sems(send_sem, recv_sem)

    def dev(seq, head=None):
        return {"seq": seq, "head": mx if head is None else head}

    def at(yy, zz, cc):
        return yy * 8 + zz * 2 + cc

    sib = dev(s + 1 - 2 * c)
    nxt = dev((s + 2) % 32)
    prv = dev((s + 30) % 32)
    zp, zm = dev(at(y, (z + 1) % 4, c)), dev(at(y, (z + 3) % 4, c))
    yp, ym = dev(at((y + 1) % 4, z, c)), dev(at((y + 3) % 4, z, c))
    xp, xm = dev(s, (mx + 1) % 4), dev(s, (mx + 3) % 4)
    p = y * 4 + z
    fwd = dev(((y * 4 + (z + 1) % 4 + 2) % 16) * 2 + c)
    po = (p + 14) % 16
    bwd = dev(at(po // 4, (po + 3) % 4, c))
    swap = {"seq": at(mx, z, c), "head": y}
    off = mx != y
    far, plus = (mx + 2) % 4 == y, mx == (y + 1) % 4
    hop, unhop = {"seq": at((y + 3) % 4, z, c), "head": y}, {"seq": at((y + 1) % 4, z, c), "head": (mx + 2) % 4}
    relays = plus
    f1, f2 = z + c * (y - z), y + c * (z - y)

    def along(first, step):
        d1, d2 = (step, 0) if first else (0, step)
        i1, i2 = (f1 + d1) % 4, (f2 + d2) % 4
        yy, zz = i2 + c * (i1 - i2), i1 + c * (i2 - i1)
        return dev(at(yy, zz, c))

    def wblock(d1, d2):
        i1, i2 = (f1 + d1) % 4, (f2 + d2) % 4
        yy, zz = i2 + c * (i1 - i2), i1 + c * (i2 - i1)
        return wbuf.at[c, yy, zz]

    loc = []

    def local(src, dst):
        d = pltpu.make_async_copy(src, dst, loc_sem.at[len(loc)])
        d.start()
        loc.append(d)
        return d

    own = pl.ds(2048, TOK)
    lk = [local(k_ref.at[:, pl.ds(j * DH, DH)], kd.at[j, own]) for j in range(2)]
    lv = [local(v_ref.at[:, pl.ds(j * DH, DH)], vd.at[j, own]) for j in range(2)]
    lq = [local(q_ref.at[:, pl.ds(h * DH, DH)], qd.at[h]) for h in range(8)]

    barrier = pltpu.get_barrier_semaphore()
    for peer in (sib, nxt, prv, zp, zm, yp, ym, xp, xm, fwd, bwd):
        pl.semaphore_signal(barrier, inc=1, device_id=peer, device_id_type=MESH)

    @pl.when(off & jnp.logical_not(far))
    def _():
        pl.semaphore_signal(barrier, inc=1, device_id=swap, device_id_type=MESH)

    @pl.when(far)
    def _():
        pl.semaphore_signal(barrier, inc=1, device_id=hop, device_id_type=MESH)

    @pl.when(relays)
    def _():
        pl.semaphore_signal(barrier, inc=1, device_id=unhop, device_id_type=MESH)

    lens[...] = jnp.zeros_like(lens)
    lens[0:1, 0:64] = len_ref[...]
    row = lens[0:1, :].astype(F32)
    i0 = lax.broadcasted_iota(jnp.int32, (DH, DH), 0)
    i1 = lax.broadcasted_iota(jnp.int32, (DH, DH), 1)
    col = jnp.sum(jnp.where(i1 < i0, jnp.broadcast_to(row, (DH, DH)), 0.0), axis=1, keepdims=True)
    start = jnp.sum(jnp.where(i0 == i1, jnp.broadcast_to(col, (DH, DH)), 0.0), axis=0, keepdims=True)
    end = start + row
    first = s * TOK

    @pl.loop(0, ROWS // 256)
    def _(b):
        pos = (first - 2048 + b * 256 + lax.broadcasted_iota(jnp.int32, (256, DH), 0)).astype(F32)
        inside = (pos >= start) & (pos < end)
        kcode[pl.ds(pl.multiple_of(b * 256, 256), 256), :] = jnp.where(inside, 0.0, -FAR).astype(BF16)

    for b in range(2):
        pos = (first + b * 256 + lax.broadcasted_iota(jnp.int32, (256, DH), 0)).astype(F32)
        inside = (pos >= start) & (pos < end)
        qcode[pl.ds(b * 256, 256), :] = jnp.where(inside, 1.0, 0.0).astype(BF16)

    for d in lk + lv:
        d.wait()
    pl.semaphore_wait(barrier, 11 + off.astype(jnp.int32) + relays.astype(jnp.int32))

    def slot(buf, j, i):
        start_row = (4 - i) * TOK
        if not isinstance(i, int):
            start_row = pl.multiple_of(start_row, TOK)
        return buf.at[j, pl.ds(start_row, TOK)]

    def both(name, j, src, dst, to):
        sm.go(f"{name}k{j}", slot(kd, j, src), slot(kd, j, dst), to)
        sm.go(f"{name}v{j}", slot(vd, j, src), slot(vd, j, dst), to)

    def both_recv(name, j, dst):
        sm.remote(f"{name}k{j}", slot(kd, j, dst), slot(kd, j, dst), sib).wait_recv()
        sm.remote(f"{name}v{j}", slot(vd, j, dst), slot(vd, j, dst), sib).wait_recv()

    def side(name, j, src, dst, when):
        ds = [sm.remote(f"{name}k{j}", slot(kd, j, src), slot(kd, j, dst), sib),
              sm.remote(f"{name}v{j}", slot(vd, j, src), slot(vd, j, dst), sib)]

        @pl.when(when)
        def _():
            for d in ds:
                d.start()
        return ds

    def kv_near(j):
        sm.go(f"relay{j}", slot(vd, j, 0), vrelay.at[j], zm)
        both("near", j, 0, 2, nxt)
        side("d1", j, 0, 1, c == 0)

    def kv_fwd(j):
        sm.remote(f"relay{j}", vrelay.at[j], vrelay.at[j], sib).wait_recv()
        sm.go(f"farv{j}", vrelay.at[j], slot(vd, j, 4), fwd)

    def kv_mid(j):
        sm.remote(f"neark{j}", slot(kd, j, 2), slot(kd, j, 2), sib).wait_recv()
        sm.go(f"fark{j}", slot(kd, j, 2), slot(kd, j, 4), nxt)

    def kv_side(j):
        sm.remote(f"nearv{j}", slot(vd, j, 2), slot(vd, j, 2), sib).wait_recv()
        side("d1", j, 2, 1, c == 1)
        side("d2", j, 2, 3, c == 0)

    def kv_last(j):
        sm.remote(f"fark{j}", slot(kd, j, 4), slot(kd, j, 4), sib).wait_recv()
        sm.remote(f"farv{j}", slot(vd, j, 4), slot(vd, j, 4), sib).wait_recv()
        side("d2", j, 4, 3, c == 1)

    ones = jnp.ones((256, DH), BF16)

    def tile(h, j, qc, lo, n, init, diag, last):
        rows = pl.ds(qc * 256, 256)
        qa = jnp.concatenate([qd[h, rows, :], qcode[rows, :]], axis=1)
        ka = jnp.concatenate([kd[j, pl.ds(lo, n), :], kcode[pl.ds(lo, n), :]], axis=1)
        sc = lax.dot_general(qa, ka, (((1,), (1,)), ((), ())), preferred_element_type=F32)
        if diag:
            r = lax.broadcasted_iota(jnp.int32, (256, n), 0)
            u = lax.broadcasted_iota(jnp.int32, (256, n), 1)
            sc = jnp.where(u <= r + qc * 256, sc, -FAR)
        top = jnp.max(sc, axis=1, keepdims=True)
        if init:
            new = jnp.broadcast_to(top, (256, DH))
        else:
            old = mbuf[h, rows, :]
            new = jnp.maximum(old, top)
        pr = jnp.exp2((sc - jnp.concatenate([new] * (n // DH), axis=1)) * C2).astype(BF16)
        va = jnp.concatenate(
            [vd[j, pl.ds(lo, n), :], jnp.concatenate([ones] * (n // 256), axis=0)], axis=1)
        o = jnp.dot(pr, va, preferred_element_type=F32)
        if not init:
            fade = jnp.exp2((old - new) * C2)
            o = o + acc[h, rows, :] * jnp.concatenate([fade, fade], axis=1)
        if last:
            abuf[mx, h, rows, :] = (o[:, :DH] / o[:, DH:]).astype(BF16)
        else:
            mbuf[h, rows, :] = new
            acc[h, rows, :] = o

    def sweep(j, step, after=None, hooks=()):
        @pl.loop(0, 4)
        def _(g):
            h = j * 4 + g
            for qc in range(2):
                if step == 0:
                    tile(h, j, qc, 2048, 256 + 256 * qc, True, True, False)
                elif step == 1:
                    tile(h, j, qc, 1024, 1024, False, False, False)
                else:
                    tile(h, j, qc, 256 * qc, 1024 - 256 * qc, False, False, True)
            if after is not None:
                after(h)
            for when, steps in hooks:
                @pl.when(g == when)
                def _():
                    for name, *args in steps:
                        name(*args)

    def xcopy(kind, h, block, lo, n, to):
        ref = abuf.at[block, h, pl.ds(lo, n)]
        return pltpu.make_async_remote_copy(
            src_ref=ref, dst_ref=ref, send_sem=xs_sem.at[kind, h], recv_sem=xr_sem.at[kind, h],
            device_id=to, device_id_type=MESH)

    xl, xr, xo = (mx + 3) % 4, (mx + 1) % 4, (mx + 2) % 4

    def xsend(h):
        xcopy(0, h, mx, 0, TOK, xp).start()
        xcopy(1, h, mx, 0, TOK, xm).start()

    def xrelay(h):
        xcopy(0, h, xl, 0, TOK, xp).wait_recv()
        xcopy(2, h, xl, 0, 256, xp).start()
        xcopy(1, h, xr, 0, TOK, xm).wait_recv()
        xcopy(3, h, xr, 256, 256, xm).start()

    def xdone(h):
        xcopy(2, h, xo, 0, 256, xp).wait_recv()
        xcopy(3, h, xo, 256, 256, xm).wait_recv()

    parts = ((0, 512), (512, 512))

    def half(ref, i):
        return ref.at[pl.ds(*parts[i])]

    def wt(i, src, dst):
        return sm.remote(f"wt{i}", half(src, i), half(dst, i), swap)

    def wl(i):
        return pltpu.make_async_copy(half(w_ref, i), half(wbuf.at[c, y, z], i), loc_sem.at[12 + i])


    def w_hop(i, src):
        return sm.remote(f"wh{i}", half(src, i), half(wrelay, i), hop)

    def w_last(i, src):
        return sm.remote(f"wz{i}", half(src, i), half(wbuf.at[c, (mx + 2) % 4, z], i), ym)

    def w_swap(last):
        @pl.when(plus if last else off & jnp.logical_not(plus | far))
        def _():
            for i in range(2):
                wt(i, w_ref, wbuf.at[c, mx, z]).start()

        if not last:
            @pl.when(far)
            def _():
                for i in range(2):
                    w_hop(i, w_ref).start()

            @pl.when(jnp.logical_not(off))
            def _():
                for i in range(2):
                    wl(i).start()

    def w_passed(i):
        @pl.when(relays)
        def _():
            w_hop(i, wrelay).wait_recv()
            w_last(i, wrelay).start()

    def w_swapped(i):
        @pl.when(off & jnp.logical_not(far))
        def _():
            wt(i, wbuf.at[c, y, z], wbuf.at[c, y, z]).wait_recv()

        @pl.when(far)
        def _():
            w_last(i, wrelay).wait_recv()

        @pl.when(jnp.logical_not(off))
        def _():
            wl(i).wait()

    def w_side(d1, d2):
        b = wblock(d1, d2)
        sm.go(f"ws{d1}{d2}", b, b, sib)

    def w_send(d1, d2, second, halves=(0, 1), core=None):
        b = wblock(d1, d2)
        ds = []
        for i in halves:
            for sign, k in (("+", i), ("-", 1 - i if len(halves) == 2 else i)):
                ds.append(sm.remote(f"w{second}{sign}{d1}h{k}", half(b, k), half(b, k),
                                    along(not second, 1 if sign == "+" else -1)))
                if core in (None, 0):
                    sm.pending.append((f"w{second}{sign}{d1}h{k}", half(b, k).shape[0]))

        def start():
            for d in ds:
                d.start()

        if core is None:
            start()
        else:
            pl.when(c == core)(start)

    def w_got(sign, d1, second, i, b):
        sm.remote(f"w{second}{sign}{d1}h{i}", half(b, i), half(b, i), sib).wait_recv()

    def w_pair(d1, second):
        a, b = ((d1, -1), (d1, 1)) if second else ((-1, 0), (1, 0))
        return a, b

    def w_relay(d1, second):
        a, b = w_pair(d1, second)
        ra, rb = wblock(*a), wblock(*b)
        w_got("+", d1, second, 0, ra)
        sm.go(f"wr{second}+{d1}", half(ra, 0), half(ra, 0), along(not second, 1))
        w_got("-", d1, second, 1, rb)
        sm.go(f"wr{second}-{d1}", half(rb, 1), half(rb, 1), along(not second, -1))

    def w_rest(d1, second):
        a, b = w_pair(d1, second)
        w_got("+", d1, second, 1, wblock(*a))
        w_side(*a)
        w_got("-", d1, second, 0, wblock(*b))
        w_side(*b)

    def w_far(d1, second):
        o = (d1, 2) if second else (2, 0)
        b = wblock(*o)
        sm.remote(f"wr{second}+{d1}", half(b, 0), half(b, 0), sib).wait_recv()
        sm.remote(f"wr{second}-{d1}", half(b, 1), half(b, 1), sib).wait_recv()
        w_side(*o)

    def project(terms, init, last=False):
        @pl.loop(0, 2)
        def _(cc):
            a = jnp.concatenate([abuf[x, j * 4 + g] for x, j in terms for g in range(4)], axis=1)
            for b in (0, 2):
                w = jnp.concatenate(
                    [jnp.concatenate([wbuf[cc, x, b, pl.ds(j * 512, 512), :],
                                      wbuf[cc, x, b + 1, pl.ds(j * 512, 512), :]], axis=1)
                     for x, j in terms], axis=0)
                o = jnp.dot(a, w, preferred_element_type=F32)
                if not init:
                    o = o + oacc[cc, b // 2]
                if last:
                    for i in range(2):
                        cols = pl.ds(pl.multiple_of((2 * (b + i) + cc) * 128, 128), 128)
                        out_ref[:, cols] = o[:, i * 128:(i + 1) * 128].astype(BF16)
                else:
                    oacc[cc, b // 2] = o

    kv_near(0)
    w_swap(False)
    for d in lq:
        d.wait()
    sweep(0, 0)
    sweep(1, 0)
    kv_mid(0)
    kv_fwd(0)
    w_swap(True)
    kv_side(0)
    both_recv("d1", 0, 1)
    sweep(0, 1)
    w_passed(0)
    w_passed(1)
    kv_near(1)
    kv_last(0)
    both_recv("d2", 0, 3)
    sweep(0, 2, xsend)
    w_swapped(0)
    w_swapped(1)
    w_send(0, 0, 0)
    w_send(0, 0, 1, (0, 1), 0)
    w_side(0, 0)
    kv_fwd(1)
    kv_mid(1)
    kv_side(1)
    both_recv("d1", 1, 1)
    sweep(1, 1, None, (
        (2, ((w_relay, 0, 0), (w_rest, 0, 0),
             (w_send, 1, 0, 1, (0, 1), 0), (w_send, -1, 0, 1, (0, 1), 0),
             (w_send, 0, 0, 1, (0, 1), 1), (w_send, 1, 0, 1, (0, 1), 1), (w_send, -1, 0, 1, (0, 1), 1))),
        (3, ((xrelay, 0),)),
    ))
    kv_last(1)
    both_recv("d2", 1, 3)
    sweep(1, 2, xsend, (
        (0, ((w_far, 0, 0), (w_send, 2, 0, 1))),
        (1, ((xrelay, 1),)),
        (3, ((xrelay, 2),)),
    ))
    w_relay(0, 1)
    w_relay(1, 1)
    xrelay(3)
    w_relay(-1, 1)
    xrelay(4)
    w_rest(0, 1)
    w_rest(1, 1)
    w_rest(-1, 1)
    xrelay(5)
    w_relay(2, 1)
    xrelay(6)
    w_far(0, 1)
    w_rest(2, 1)
    xrelay(7)
    w_far(1, 1)
    w_far(-1, 1)
    w_far(2, 1)
    for d1 in (0, -1, 1, 2):
        for d2 in (0, -1, 1, 2):
            sm.remote(f"ws{d1}{d2}", wbuf.at[1 - c, 0, 0], wbuf.at[1 - c, 0, 0], sib).wait_recv()
    project([(mx, 0), (mx, 1)], True)
    project([(xl, 0), (xr, 0)], False)
    for h in range(4):
        xdone(h)
    project([(xo, 0), (xl, 1), (xr, 1)], False)
    for h in range(4, 8):
        xdone(h)
    project([(xo, 1)], False, True)

    for name, n in sm.pending:
        ref = wrelay.at[pl.ds(0, n)]
        sm.remote(name, ref, ref, sib).wait_send()
    for j in range(2):
        for kv in "kv":
            buf = kd if kv == "k" else vd
            r = slot(buf, j, 0)
            sm.remote(f"d1{kv}{j}", r, r, sib).wait_send()
            sm.remote(f"d2{kv}{j}", r, r, sib).wait_send()

    @pl.when(off)
    def _():
        @pl.when(jnp.logical_not(far))
        def _():
            for i in range(2):
                wt(i, w_ref, wbuf.at[c, mx, z]).wait_send()

    @pl.when(far)
    def _():
        for i in range(2):
            w_hop(i, w_ref).wait_send()

    @pl.when(relays)
    def _():
        for i in range(2):
            w_last(i, wrelay).wait_send()
    for h in range(8):
        xcopy(0, h, mx, 0, TOK, xp).wait_send()
        xcopy(1, h, mx, 0, TOK, xm).wait_send()
        xcopy(2, h, xl, 0, 256, xp).wait_send()
        xcopy(3, h, xr, 256, 256, xm).wait_send()


def body(queries, keys, values, doc_lengths, out_weight):
    hbm = pl.BlockSpec(memory_space=pl.ANY)
    vmem = pl.BlockSpec(memory_space=pltpu.VMEM)
    return pl.pallas_call(
        kernel,
        out_shape=jax.ShapeDtypeStruct((TOK, 1024), BF16),
        in_specs=[hbm, hbm, hbm, hbm, vmem],
        out_specs=vmem,
        scratch_shapes=[
            pltpu.VMEM((8, TOK, DH), BF16),
            pltpu.VMEM((TOK, DH), BF16),
            pltpu.VMEM((2, ROWS, DH), BF16),
            pltpu.VMEM((ROWS, DH), BF16),
            pltpu.VMEM((2, ROWS, DH), BF16),
            pltpu.VMEM((2, TOK, DH), BF16),
            pltpu.VMEM((1024, DH), BF16),
            pltpu.VMEM((2, 4, 4, 1024, DH), BF16),
            pltpu.VMEM((4, 8, TOK, DH), BF16),
            pltpu.VMEM((8, TOK, DH), F32),
            pltpu.VMEM((8, TOK, 2 * DH), F32),
            pltpu.VMEM((2, 2, TOK, 256), F32),
            pltpu.VMEM((8, DH), jnp.int32),
            pltpu.SemaphoreType.DMA((14,)),
            pltpu.SemaphoreType.DMA((96,)),
            pltpu.SemaphoreType.DMA((96,)),
            pltpu.SemaphoreType.DMA((4, 8)),
            pltpu.SemaphoreType.DMA((4, 8)),
        ],
        compiler_params=pltpu.CompilerParams(
            collective_id=0, has_side_effects=True, vmem_limit_bytes=60 * 1024 * 1024),
        name="attention_block",
    )(queries, keys, values, out_weight, doc_lengths.reshape(1, 64))


def solution(mesh):
    return jax.shard_map(
        body,
        mesh=mesh,
        in_specs=(P("seq", "head"), P("seq", "head"), P("seq", "head"), P(), P("head", "seq")),
        out_specs=P("seq", "head"),
        check_vma=False,
    )
```

```python
import jax
import jax.numpy as jnp
from jax import lax
from jax.experimental import pallas as pl
from jax.experimental.pallas import tpu as pltpu
from jax.sharding import PartitionSpec as P

DH = 128
TOK = 512
ROWS = 2560
FAR = 16384.0
LOG2E = 1.4426950408889634
C2 = LOG2E * DH ** -0.5
F32 = jnp.float32
BF16 = jnp.bfloat16
MESH = pl.DeviceIdType.MESH


class Sems:
    def __init__(self, send, recv):
        self.send, self.recv, self.names, self.pending = send, recv, {}, []

    def index(self, name):
        return self.names.setdefault(name, len(self.names))

    def remote(self, name, src, dst, dev):
        i = self.index(name)
        return pltpu.make_async_remote_copy(
            src_ref=src, dst_ref=dst, send_sem=self.send.at[i], recv_sem=self.recv.at[i],
            device_id=dev, device_id_type=MESH)

    def go(self, name, src, dst, dev):
        self.remote(name, src, dst, dev).start()
        self.pending.append((name, src.shape[0] * src.shape[1] // DH))


def kernel(q_ref, k_ref, v_ref, w_ref, len_ref, out_ref,
           qd, qcode, kd, kcode, vown, vd, vrelay, wrelay, wbuf, abuf, mbuf, acc, s0, s1, s2, s3, t0, t1, t2, t3, oacc, lens,
           loc_sem, send_sem, recv_sem, xs_sem, xr_sem):
    mx = lax.axis_index("head")
    s = lax.axis_index("seq")
    y = s // 8
    z = (s // 2) % 4
    c = s % 2
    sm = Sems(send_sem, recv_sem)

    def dev(seq, head=None):
        return {"seq": seq, "head": mx if head is None else head}

    def at(yy, zz, cc):
        return yy * 8 + zz * 2 + cc

    sib = dev(s + 1 - 2 * c)
    nxt = dev((s + 2) % 32)
    prv = dev((s + 30) % 32)
    zp, zm = dev(at(y, (z + 1) % 4, c)), dev(at(y, (z + 3) % 4, c))
    yp, ym = dev(at((y + 1) % 4, z, c)), dev(at((y + 3) % 4, z, c))
    xp, xm = dev(s, (mx + 1) % 4), dev(s, (mx + 3) % 4)
    p = y * 4 + z
    fwd = dev(((y * 4 + (z + 1) % 4 + 2) % 16) * 2 + c)
    po = (p + 14) % 16
    bwd = dev(at(po // 4, (po + 3) % 4, c))
    swap = {"seq": at(mx, z, c), "head": y}
    off = mx != y
    far, plus = (mx + 2) % 4 == y, mx == (y + 1) % 4
    hop, unhop = {"seq": at((y + 3) % 4, z, c), "head": y}, {"seq": at((y + 1) % 4, z, c), "head": (mx + 2) % 4}
    relays = plus
    f1, f2 = z + c * (y - z), y + c * (z - y)

    def along(first, step):
        d1, d2 = (step, 0) if first else (0, step)
        i1, i2 = (f1 + d1) % 4, (f2 + d2) % 4
        yy, zz = i2 + c * (i1 - i2), i1 + c * (i2 - i1)
        return dev(at(yy, zz, c))

    def wblock(d1, d2):
        i1, i2 = (f1 + d1) % 4, (f2 + d2) % 4
        yy, zz = i2 + c * (i1 - i2), i1 + c * (i2 - i1)
        return wbuf.at[c, yy, zz]

    loc = []

    def local(src, dst):
        d = pltpu.make_async_copy(src, dst, loc_sem.at[len(loc)])
        d.start()
        loc.append(d)
        return d

    own = pl.ds(2048, TOK)
    lk = [local(k_ref.at[:, pl.ds(j * DH, DH)], kd.at[j, own]) for j in range(2)]
    lv = [local(v_ref.at[:, pl.ds(j * DH, DH)], vown.at[j]) for j in range(2)]
    lq = [local(q_ref.at[:, pl.ds(h * DH, DH)], qd.at[h]) for h in range(8)]

    barrier = pltpu.get_barrier_semaphore()
    for peer in (sib, nxt, prv, zp, zm, yp, ym, xp, xm, fwd, bwd):
        pl.semaphore_signal(barrier, inc=1, device_id=peer, device_id_type=MESH)

    @pl.when(off & jnp.logical_not(far))
    def _():
        pl.semaphore_signal(barrier, inc=1, device_id=swap, device_id_type=MESH)

    @pl.when(far)
    def _():
        pl.semaphore_signal(barrier, inc=1, device_id=hop, device_id_type=MESH)

    @pl.when(relays)
    def _():
        pl.semaphore_signal(barrier, inc=1, device_id=unhop, device_id_type=MESH)

    lens[...] = jnp.zeros_like(lens)
    lens[0:1, 0:64] = len_ref[...]
    row = lens[0:1, :].astype(F32)
    i0 = lax.broadcasted_iota(jnp.int32, (DH, DH), 0)
    i1 = lax.broadcasted_iota(jnp.int32, (DH, DH), 1)
    col = jnp.sum(jnp.where(i1 < i0, jnp.broadcast_to(row, (DH, DH)), 0.0), axis=1, keepdims=True)
    start = jnp.sum(jnp.where(i0 == i1, jnp.broadcast_to(col, (DH, DH)), 0.0), axis=0, keepdims=True)
    end = start + row
    first = s * TOK

    @pl.loop(0, ROWS // 256)
    def _(b):
        pos = (first - 2048 + b * 256 + lax.broadcasted_iota(jnp.int32, (256, DH), 0)).astype(F32)
        inside = (pos >= start) & (pos < end)
        kcode[pl.ds(pl.multiple_of(b * 256, 256), 256), :] = jnp.where(inside, 0.0, -FAR).astype(BF16)

    for b in range(2):
        pos = (first + b * 256 + lax.broadcasted_iota(jnp.int32, (256, DH), 0)).astype(F32)
        inside = (pos >= start) & (pos < end)
        qcode[pl.ds(b * 256, 256), :] = jnp.where(inside, 1.0, 0.0).astype(BF16)

    for d in lk + lv:
        d.wait()
    for j in range(2):
        vd[j, 4] = vown[j].T
    pl.semaphore_wait(barrier, 11 + off.astype(jnp.int32) + relays.astype(jnp.int32))

    def slot(buf, j, i):
        if buf is vd:
            return vd.at[j, 4 - i]
        start_row = (4 - i) * TOK
        if not isinstance(i, int):
            start_row = pl.multiple_of(start_row, TOK)
        return buf.at[j, pl.ds(start_row, TOK)]

    def both(name, j, src, dst, to):
        sm.go(f"{name}k{j}", slot(kd, j, src), slot(kd, j, dst), to)
        sm.go(f"{name}v{j}", slot(vd, j, src), slot(vd, j, dst), to)

    def both_recv(name, j, dst):
        sm.remote(f"{name}k{j}", slot(kd, j, dst), slot(kd, j, dst), sib).wait_recv()
        sm.remote(f"{name}v{j}", slot(vd, j, dst), slot(vd, j, dst), sib).wait_recv()

    def side(name, j, src, dst, when):
        ds = [sm.remote(f"{name}k{j}", slot(kd, j, src), slot(kd, j, dst), sib),
              sm.remote(f"{name}v{j}", slot(vd, j, src), slot(vd, j, dst), sib)]

        @pl.when(when)
        def _():
            for d in ds:
                d.start()
        return ds

    def kv_near(j):
        sm.go(f"relay{j}", slot(vd, j, 0), vrelay.at[j], zm)
        both("near", j, 0, 2, nxt)
        side("d1", j, 0, 1, c == 0)

    def kv_fwd(j):
        sm.remote(f"relay{j}", vrelay.at[j], vrelay.at[j], sib).wait_recv()
        sm.go(f"farv{j}", vrelay.at[j], slot(vd, j, 4), fwd)

    def kv_mid(j):
        sm.remote(f"neark{j}", slot(kd, j, 2), slot(kd, j, 2), sib).wait_recv()
        sm.go(f"fark{j}", slot(kd, j, 2), slot(kd, j, 4), nxt)

    def kv_side(j):
        sm.remote(f"nearv{j}", slot(vd, j, 2), slot(vd, j, 2), sib).wait_recv()
        side("d1", j, 2, 1, c == 1)
        side("d2", j, 2, 3, c == 0)

    def kv_last(j):
        sm.remote(f"fark{j}", slot(kd, j, 4), slot(kd, j, 4), sib).wait_recv()
        sm.remote(f"farv{j}", slot(vd, j, 4), slot(vd, j, 4), sib).wait_recv()
        side("d2", j, 4, 3, c == 1)

    CK, WK = 1024, 256

    def scores(h, j, qc, lo, n, diag, sref, tref):
        rows = pl.ds(qc * 256, 256)
        qa = jnp.concatenate([qd[h, rows, :], qcode[rows, :]], axis=1)
        top = None
        for at_key in range(0, n, CK):
            m = min(CK, n - at_key)
            keys = pl.ds(lo + at_key, m)
            ka = jnp.concatenate([kd[j, keys, :], kcode[keys, :]], axis=1)
            sc = lax.dot_general(ka, qa, (((1,), (1,)), ((), ())), preferred_element_type=F32)
            if diag:
                u = at_key + lax.broadcasted_iota(jnp.int32, (m, 256), 0)
                r = lax.broadcasted_iota(jnp.int32, (m, 256), 1)
                sc = jnp.where(u <= r + qc * 256, sc, -FAR)
            sref[at_key:at_key + m, :] = sc
            best = jnp.max(sc.reshape(m // 8, 8, 256), axis=0)
            top = best if top is None else jnp.maximum(top, best)
            yield
        tref[...] = jnp.broadcast_to(jnp.max(top, axis=0, keepdims=True), (8, 256))

    def weigh(h, j, qc, lo, n, init, last, sref, tref):
        rows = pl.ds(qc * 256, 256)
        new = tref[0:1, :]
        if not init:
            old = mbuf[h, qc, 0:1, :]
            new = jnp.maximum(old, new)
            o = acc[h, qc] * jnp.exp2((old - new) * C2)
        at_key = lo
        while at_key < lo + n:
            m = min(WK, lo + n - at_key, TOK - at_key % TOK)
            pr = jnp.exp2((sref[pl.ds(at_key - lo, m), :] - new) * C2).astype(BF16)
            va = jnp.concatenate(
                [vd[j, at_key // TOK, :, pl.ds(at_key % TOK, m)], jnp.ones((16, m), BF16)], axis=0)
            part = jnp.dot(va, pr, preferred_element_type=F32)
            o = part if init and at_key == lo else o + part
            at_key += m
            yield
        if last:
            abuf[mx, h, rows, :] = (o[:DH] / o[DH:DH + 1]).T.astype(BF16)
        else:
            mbuf[h, qc] = jnp.broadcast_to(new, (8, 256))
            acc[h, qc] = o

    def interleave(*streams):
        live = list(streams)
        while live:
            live = [s for s in live if next(s, live) is not live]

    def sweep(j, step, after=None, hooks=()):
        init, last = step == 0, step == 2
        spans = {0: ((2048, 256), (2048, 512)), 1: ((1024, 1024), (1024, 1024)), 2: ((0, 1024), (256, 768))}[step]
        bufs = ((s0, s1), (s2, s3)), ((t0, t1), (t2, t3))

        def make(g):
            return [scores(j * 4 + g, j, qc, *spans[qc], init, bufs[0][g % 2][qc], bufs[1][g % 2][qc])
                    for qc in range(2)]

        def use(g):
            return [weigh(j * 4 + g, j, qc, *spans[qc], init, last, bufs[0][g % 2][qc], bufs[1][g % 2][qc])
                    for qc in range(2)]

        interleave(*make(0))
        for g in range(4):
            interleave(*(make(g + 1) if g < 3 else []), *use(g))
            if after is not None:
                after(j * 4 + g)
            for when, steps in hooks:
                if when == g:
                    for name, *args in steps:
                        name(*args)

    def xcopy(kind, h, block, lo, n, to):
        ref = abuf.at[block, h, pl.ds(lo, n)]
        return pltpu.make_async_remote_copy(
            src_ref=ref, dst_ref=ref, send_sem=xs_sem.at[kind, h], recv_sem=xr_sem.at[kind, h],
            device_id=to, device_id_type=MESH)

    xl, xr, xo = (mx + 3) % 4, (mx + 1) % 4, (mx + 2) % 4

    def xsend(h):
        xcopy(0, h, mx, 0, TOK, xp).start()
        xcopy(1, h, mx, 0, TOK, xm).start()

    def xrelay(h):
        xcopy(0, h, xl, 0, TOK, xp).wait_recv()
        xcopy(2, h, xl, 0, 256, xp).start()
        xcopy(1, h, xr, 0, TOK, xm).wait_recv()
        xcopy(3, h, xr, 256, 256, xm).start()

    def xdone(h):
        xcopy(2, h, xo, 0, 256, xp).wait_recv()
        xcopy(3, h, xo, 256, 256, xm).wait_recv()

    parts = ((0, 512), (512, 512))

    def half(ref, i):
        return ref.at[pl.ds(*parts[i])]

    def wt(i, src, dst):
        return sm.remote(f"wt{i}", half(src, i), half(dst, i), swap)

    def wl(i):
        return pltpu.make_async_copy(half(w_ref, i), half(wbuf.at[c, y, z], i), loc_sem.at[12 + i])


    def w_hop(i, src):
        return sm.remote(f"wh{i}", half(src, i), half(wrelay, i), hop)

    def w_last(i, src):
        return sm.remote(f"wz{i}", half(src, i), half(wbuf.at[c, (mx + 2) % 4, z], i), ym)

    def w_swap(last):
        @pl.when(plus if last else off & jnp.logical_not(plus | far))
        def _():
            for i in range(2):
                wt(i, w_ref, wbuf.at[c, mx, z]).start()

        if not last:
            @pl.when(far)
            def _():
                for i in range(2):
                    w_hop(i, w_ref).start()

            @pl.when(jnp.logical_not(off))
            def _():
                for i in range(2):
                    wl(i).start()

    def w_passed(i):
        @pl.when(relays)
        def _():
            w_hop(i, wrelay).wait_recv()
            w_last(i, wrelay).start()

    def w_swapped(i):
        @pl.when(off & jnp.logical_not(far))
        def _():
            wt(i, wbuf.at[c, y, z], wbuf.at[c, y, z]).wait_recv()

        @pl.when(far)
        def _():
            w_last(i, wrelay).wait_recv()

        @pl.when(jnp.logical_not(off))
        def _():
            wl(i).wait()

    def w_side(d1, d2):
        b = wblock(d1, d2)
        sm.go(f"ws{d1}{d2}", b, b, sib)

    def w_send(d1, d2, second, halves=(0, 1), core=None):
        b = wblock(d1, d2)
        ds = []
        for i in halves:
            for sign, k in (("+", i), ("-", 1 - i if len(halves) == 2 else i)):
                ds.append(sm.remote(f"w{second}{sign}{d1}h{k}", half(b, k), half(b, k),
                                    along(not second, 1 if sign == "+" else -1)))
                if core in (None, 0):
                    sm.pending.append((f"w{second}{sign}{d1}h{k}", half(b, k).shape[0]))

        def start():
            for d in ds:
                d.start()

        if core is None:
            start()
        else:
            pl.when(c == core)(start)

    def w_got(sign, d1, second, i, b):
        sm.remote(f"w{second}{sign}{d1}h{i}", half(b, i), half(b, i), sib).wait_recv()

    def w_pair(d1, second):
        a, b = ((d1, -1), (d1, 1)) if second else ((-1, 0), (1, 0))
        return a, b

    def w_relay(d1, second):
        a, b = w_pair(d1, second)
        ra, rb = wblock(*a), wblock(*b)
        w_got("+", d1, second, 0, ra)
        sm.go(f"wr{second}+{d1}", half(ra, 0), half(ra, 0), along(not second, 1))
        w_got("-", d1, second, 1, rb)
        sm.go(f"wr{second}-{d1}", half(rb, 1), half(rb, 1), along(not second, -1))

    def w_rest(d1, second):
        a, b = w_pair(d1, second)
        w_got("+", d1, second, 1, wblock(*a))
        w_side(*a)
        w_got("-", d1, second, 0, wblock(*b))
        w_side(*b)

    def w_far(d1, second):
        o = (d1, 2) if second else (2, 0)
        b = wblock(*o)
        sm.remote(f"wr{second}+{d1}", half(b, 0), half(b, 0), sib).wait_recv()
        sm.remote(f"wr{second}-{d1}", half(b, 1), half(b, 1), sib).wait_recv()
        w_side(*o)

    def project(terms, init, last=False):
        @pl.loop(0, 2)
        def _(cc):
            a = jnp.concatenate([abuf[x, j * 4 + g] for x, j in terms for g in range(4)], axis=1)
            for b in (0, 2):
                w = jnp.concatenate(
                    [jnp.concatenate([wbuf[cc, x, b, pl.ds(j * 512, 512), :],
                                      wbuf[cc, x, b + 1, pl.ds(j * 512, 512), :]], axis=1)
                     for x, j in terms], axis=0)
                o = jnp.dot(a, w, preferred_element_type=F32)
                if not init:
                    o = o + oacc[cc, b // 2]
                if last:
                    for i in range(2):
                        cols = pl.ds(pl.multiple_of((2 * (b + i) + cc) * 128, 128), 128)
                        out_ref[:, cols] = o[:, i * 128:(i + 1) * 128].astype(BF16)
                else:
                    oacc[cc, b // 2] = o

    kv_near(0)
    w_swap(False)
    for d in lq:
        d.wait()
    sweep(0, 0)
    sweep(1, 0)
    kv_mid(0)
    kv_fwd(0)
    kv_side(0)
    w_swap(True)
    both_recv("d1", 0, 1)
    sweep(0, 1)
    w_passed(0)
    w_passed(1)
    kv_near(1)
    kv_last(0)
    both_recv("d2", 0, 3)
    sweep(0, 2, xsend)
    w_swapped(0)
    w_swapped(1)
    w_send(0, 0, 0)
    w_send(0, 0, 1, (0, 1), 0)
    w_side(0, 0)
    kv_fwd(1)
    kv_mid(1)
    kv_side(1)
    both_recv("d1", 1, 1)
    sweep(1, 1, None, (
        (2, ((w_relay, 0, 0), (w_rest, 0, 0),
             (w_send, 1, 0, 1, (0, 1), 0), (w_send, -1, 0, 1, (0, 1), 0),
             (w_send, 0, 0, 1, (0, 1), 1), (w_send, 1, 0, 1, (0, 1), 1), (w_send, -1, 0, 1, (0, 1), 1))),
        (3, ((xrelay, 0),)),
    ))
    kv_last(1)
    both_recv("d2", 1, 3)
    sweep(1, 2, xsend, (
        (0, ((w_far, 0, 0), (w_send, 2, 0, 1))),
        (1, ((xrelay, 1),)),
        (3, ((xrelay, 2),)),
    ))
    w_relay(0, 1)
    w_relay(1, 1)
    xrelay(3)
    w_relay(-1, 1)
    xrelay(4)
    w_rest(0, 1)
    w_rest(1, 1)
    w_rest(-1, 1)
    xrelay(5)
    w_relay(2, 1)
    xrelay(6)
    w_far(0, 1)
    w_rest(2, 1)
    xrelay(7)
    w_far(1, 1)
    w_far(-1, 1)
    w_far(2, 1)
    for d1 in (0, -1, 1, 2):
        for d2 in (0, -1, 1, 2):
            sm.remote(f"ws{d1}{d2}", wbuf.at[1 - c, 0, 0], wbuf.at[1 - c, 0, 0], sib).wait_recv()
    project([(mx, 0), (mx, 1)], True)
    project([(xl, 0), (xr, 0)], False)
    for h in range(4):
        xdone(h)
    project([(xo, 0), (xl, 1), (xr, 1)], False)
    for h in range(4, 8):
        xdone(h)
    project([(xo, 1)], False, True)

    for name, n in sm.pending:
        ref = wrelay.at[pl.ds(0, n)]
        sm.remote(name, ref, ref, sib).wait_send()
    for j in range(2):
        for kv in "kv":
            buf = kd if kv == "k" else vd
            r = slot(buf, j, 0)
            sm.remote(f"d1{kv}{j}", r, r, sib).wait_send()
            sm.remote(f"d2{kv}{j}", r, r, sib).wait_send()

    @pl.when(off)
    def _():
        @pl.when(jnp.logical_not(far))
        def _():
            for i in range(2):
                wt(i, w_ref, wbuf.at[c, mx, z]).wait_send()

    @pl.when(far)
    def _():
        for i in range(2):
            w_hop(i, w_ref).wait_send()

    @pl.when(relays)
    def _():
        for i in range(2):
            w_last(i, wrelay).wait_send()
    for h in range(8):
        xcopy(0, h, mx, 0, TOK, xp).wait_send()
        xcopy(1, h, mx, 0, TOK, xm).wait_send()
        xcopy(2, h, xl, 0, 256, xp).wait_send()
        xcopy(3, h, xr, 256, 256, xm).wait_send()


def body(queries, keys, values, doc_lengths, out_weight):
    hbm = pl.BlockSpec(memory_space=pl.ANY)
    vmem = pl.BlockSpec(memory_space=pltpu.VMEM)
    return pl.pallas_call(
        kernel,
        out_shape=pltpu.VMEM((TOK, 1024), BF16),
        in_specs=[hbm, hbm, hbm, hbm, vmem],
        out_specs=vmem,
        scratch_shapes=[
            pltpu.VMEM((8, TOK, DH), BF16),
            pltpu.VMEM((TOK, DH), BF16),
            pltpu.VMEM((2, ROWS, DH), BF16),
            pltpu.VMEM((ROWS, DH), BF16),
            pltpu.VMEM((2, TOK, DH), BF16),
            pltpu.VMEM((2, 5, DH, TOK), BF16),
            pltpu.VMEM((2, DH, TOK), BF16),
            pltpu.VMEM((1024, DH), BF16),
            pltpu.VMEM((2, 4, 4, 1024, DH), BF16),
            pltpu.VMEM((4, 8, TOK, DH), BF16),
            pltpu.VMEM((8, 2, 8, 256), F32),
            pltpu.VMEM((8, 2, DH + 16, 256), F32),
            *[pltpu.VMEM((1024, 256), F32)] * 4,
            *[pltpu.VMEM((8, 256), F32)] * 4,
            pltpu.VMEM((2, 2, TOK, 256), F32),
            pltpu.VMEM((8, DH), jnp.int32),
            pltpu.SemaphoreType.DMA((14,)),
            pltpu.SemaphoreType.DMA((96,)),
            pltpu.SemaphoreType.DMA((96,)),
            pltpu.SemaphoreType.DMA((4, 8)),
            pltpu.SemaphoreType.DMA((4, 8)),
        ],
        compiler_params=pltpu.CompilerParams(
            collective_id=0, has_side_effects=True, vmem_limit_bytes=60 * 1024 * 1024),
        name="attention_block",
    )(queries, keys, values, out_weight, doc_lengths.reshape(1, 64))


def solution(mesh):
    return jax.shard_map(
        body,
        mesh=mesh,
        in_specs=(P("seq", "head"), P("seq", "head"), P("seq", "head"), P(), P("head", "seq")),
        out_specs=P("seq", "head"),
        check_vma=False,
    )
```

```python
import jax
import jax.numpy as jnp
from jax import lax
from jax.experimental import pallas as pl
from jax.experimental.pallas import tpu as pltpu
from jax.sharding import PartitionSpec as P

DH = 128
TOK = 512
ROWS = 2560
FAR = 16384.0
LOG2E = 1.4426950408889634
C2 = LOG2E * DH ** -0.5
F32 = jnp.float32
BF16 = jnp.bfloat16
MESH = pl.DeviceIdType.MESH


class Sems:
    def __init__(self, send, recv):
        self.send, self.recv, self.names, self.pending = send, recv, {}, []

    def index(self, name):
        return self.names.setdefault(name, len(self.names))

    def remote(self, name, src, dst, dev):
        i = self.index(name)
        return pltpu.make_async_remote_copy(
            src_ref=src, dst_ref=dst, send_sem=self.send.at[i], recv_sem=self.recv.at[i],
            device_id=dev, device_id_type=MESH)

    def go(self, name, src, dst, dev):
        self.remote(name, src, dst, dev).start()
        self.pending.append((name, src.shape[0] * src.shape[1] // DH))


def kernel(q_ref, k_ref, v_ref, w_ref, len_ref, out_ref,
           qd, qcode, kd, kcode, vown, vd, vrelay, wrelay, wbuf, abuf, mbuf, acc, s0, s1, s2, s3, t0, t1, t2, t3, oacc, lens,
           loc_sem, send_sem, recv_sem, xs_sem, xr_sem):
    mx = lax.axis_index("head")
    s = lax.axis_index("seq")
    y = s // 8
    z = (s // 2) % 4
    c = s % 2
    sm = Sems(send_sem, recv_sem)

    def dev(seq, head=None):
        return {"seq": seq, "head": mx if head is None else head}

    def at(yy, zz, cc):
        return yy * 8 + zz * 2 + cc

    sib = dev(s + 1 - 2 * c)
    nxt = dev((s + 2) % 32)
    prv = dev((s + 30) % 32)
    zp, zm = dev(at(y, (z + 1) % 4, c)), dev(at(y, (z + 3) % 4, c))
    yp, ym = dev(at((y + 1) % 4, z, c)), dev(at((y + 3) % 4, z, c))
    xp, xm = dev(s, (mx + 1) % 4), dev(s, (mx + 3) % 4)
    p = y * 4 + z
    fwd = dev(((y * 4 + (z + 1) % 4 + 2) % 16) * 2 + c)
    po = (p + 14) % 16
    bwd = dev(at(po // 4, (po + 3) % 4, c))
    swap = {"seq": at(mx, z, c), "head": y}
    off = mx != y
    far, plus = (mx + 2) % 4 == y, mx == (y + 1) % 4
    hop, unhop = {"seq": at((y + 3) % 4, z, c), "head": y}, {"seq": at((y + 1) % 4, z, c), "head": (mx + 2) % 4}
    relays = plus
    f1, f2 = z + c * (y - z), y + c * (z - y)

    def along(first, step):
        d1, d2 = (step, 0) if first else (0, step)
        i1, i2 = (f1 + d1) % 4, (f2 + d2) % 4
        yy, zz = i2 + c * (i1 - i2), i1 + c * (i2 - i1)
        return dev(at(yy, zz, c))

    def wblock(d1, d2):
        i1, i2 = (f1 + d1) % 4, (f2 + d2) % 4
        yy, zz = i2 + c * (i1 - i2), i1 + c * (i2 - i1)
        return wbuf.at[c, yy, zz]

    loc = []

    def local(src, dst):
        d = pltpu.make_async_copy(src, dst, loc_sem.at[len(loc)])
        d.start()
        loc.append(d)
        return d

    own = pl.ds(2048, TOK)
    lk = [local(k_ref.at[:, pl.ds(j * DH, DH)], kd.at[j, own]) for j in range(2)]
    lv = [local(v_ref.at[:, pl.ds(j * DH, DH)], vown.at[j]) for j in range(2)]
    lq = [local(q_ref.at[:, pl.ds(h * DH, DH)], qd.at[h]) for h in range(8)]

    barrier = pltpu.get_barrier_semaphore()
    for peer in (sib, nxt, prv, zp, zm, yp, ym, xp, xm, fwd, bwd):
        pl.semaphore_signal(barrier, inc=1, device_id=peer, device_id_type=MESH)

    @pl.when(off & jnp.logical_not(far))
    def _():
        pl.semaphore_signal(barrier, inc=1, device_id=swap, device_id_type=MESH)

    @pl.when(far)
    def _():
        pl.semaphore_signal(barrier, inc=1, device_id=hop, device_id_type=MESH)

    @pl.when(relays)
    def _():
        pl.semaphore_signal(barrier, inc=1, device_id=unhop, device_id_type=MESH)

    lens[...] = jnp.zeros_like(lens)
    lens[0:1, 0:64] = len_ref[...]
    row = lens[0:1, :].astype(F32)
    i0 = lax.broadcasted_iota(jnp.int32, (DH, DH), 0)
    i1 = lax.broadcasted_iota(jnp.int32, (DH, DH), 1)
    col = jnp.sum(jnp.where(i1 < i0, jnp.broadcast_to(row, (DH, DH)), 0.0), axis=1, keepdims=True)
    start = jnp.sum(jnp.where(i0 == i1, jnp.broadcast_to(col, (DH, DH)), 0.0), axis=0, keepdims=True)
    end = start + row
    first = s * TOK

    @pl.loop(0, ROWS // 256)
    def _(b):
        pos = (first - 2048 + b * 256 + lax.broadcasted_iota(jnp.int32, (256, DH), 0)).astype(F32)
        inside = (pos >= start) & (pos < end)
        kcode[pl.ds(pl.multiple_of(b * 256, 256), 256), :] = jnp.where(inside, 0.0, -FAR).astype(BF16)

    for b in range(2):
        pos = (first + b * 256 + lax.broadcasted_iota(jnp.int32, (256, DH), 0)).astype(F32)
        inside = (pos >= start) & (pos < end)
        qcode[pl.ds(b * 256, 256), :] = jnp.where(inside, 1.0, 0.0).astype(BF16)

    for d in lk + lv:
        d.wait()
    for j in range(2):
        vd[j, 4] = vown[j].T
    pl.semaphore_wait(barrier, 11 + off.astype(jnp.int32) + relays.astype(jnp.int32))

    def slot(buf, j, i):
        if buf is vd:
            return vd.at[j, 4 - i]
        start_row = (4 - i) * TOK
        if not isinstance(i, int):
            start_row = pl.multiple_of(start_row, TOK)
        return buf.at[j, pl.ds(start_row, TOK)]

    def both(name, j, src, dst, to):
        sm.go(f"{name}k{j}", slot(kd, j, src), slot(kd, j, dst), to)
        sm.go(f"{name}v{j}", slot(vd, j, src), slot(vd, j, dst), to)

    def both_recv(name, j, dst):
        sm.remote(f"{name}k{j}", slot(kd, j, dst), slot(kd, j, dst), sib).wait_recv()
        sm.remote(f"{name}v{j}", slot(vd, j, dst), slot(vd, j, dst), sib).wait_recv()

    def side(name, j, src, dst, when):
        ds = [sm.remote(f"{name}k{j}", slot(kd, j, src), slot(kd, j, dst), sib),
              sm.remote(f"{name}v{j}", slot(vd, j, src), slot(vd, j, dst), sib)]

        @pl.when(when)
        def _():
            for d in ds:
                d.start()
        return ds

    def kv_near(j):
        sm.go(f"relay{j}", slot(vd, j, 0), vrelay.at[j], zm)
        both("near", j, 0, 2, nxt)
        side("d1", j, 0, 1, c == 0)

    def kv_fwd(j):
        sm.remote(f"relay{j}", vrelay.at[j], vrelay.at[j], sib).wait_recv()
        sm.go(f"farv{j}", vrelay.at[j], slot(vd, j, 4), fwd)

    def kv_mid(j):
        sm.remote(f"neark{j}", slot(kd, j, 2), slot(kd, j, 2), sib).wait_recv()
        sm.go(f"fark{j}", slot(kd, j, 2), slot(kd, j, 4), nxt)

    def kv_side(j):
        sm.remote(f"nearv{j}", slot(vd, j, 2), slot(vd, j, 2), sib).wait_recv()
        side("d1", j, 2, 1, c == 1)
        side("d2", j, 2, 3, c == 0)

    def kv_last(j):
        sm.remote(f"fark{j}", slot(kd, j, 4), slot(kd, j, 4), sib).wait_recv()
        sm.remote(f"farv{j}", slot(vd, j, 4), slot(vd, j, 4), sib).wait_recv()
        side("d2", j, 4, 3, c == 1)

    CK, WK = 1024, 256

    def scores(h, j, qc, lo, n, diag, sref, tref):
        rows = pl.ds(qc * 256, 256)
        qa = jnp.concatenate([qd[h, rows, :], qcode[rows, :]], axis=1)
        top = None
        for at_key in range(0, n, CK):
            m = min(CK, n - at_key)
            keys = pl.ds(lo + at_key, m)
            ka = jnp.concatenate([kd[j, keys, :], kcode[keys, :]], axis=1)
            sc = lax.dot_general(ka, qa, (((1,), (1,)), ((), ())), preferred_element_type=F32)
            if diag:
                u = at_key + lax.broadcasted_iota(jnp.int32, (m, 256), 0)
                r = lax.broadcasted_iota(jnp.int32, (m, 256), 1)
                sc = jnp.where(u <= r + qc * 256, sc, -FAR)
            sref[at_key:at_key + m, :] = sc
            best = jnp.max(sc.reshape(m // 8, 8, 256), axis=0)
            top = best if top is None else jnp.maximum(top, best)
            yield
        tref[...] = jnp.broadcast_to(jnp.max(top, axis=0, keepdims=True), (8, 256))

    def weigh(h, j, qc, lo, n, init, last, sref, tref):
        rows = pl.ds(qc * 256, 256)
        new = tref[0:1, :]
        if not init:
            old = mbuf[h, qc, 0:1, :]
            new = jnp.maximum(old, new)
            o = acc[h, qc] * jnp.exp2((old - new) * C2)
        at_key = lo
        while at_key < lo + n:
            m = min(WK, lo + n - at_key, TOK - at_key % TOK)
            pr = jnp.exp2((sref[pl.ds(at_key - lo, m), :] - new) * C2).astype(BF16)
            va = jnp.concatenate(
                [vd[j, at_key // TOK, :, pl.ds(at_key % TOK, m)], jnp.ones((16, m), BF16)], axis=0)
            part = jnp.dot(va, pr, preferred_element_type=F32)
            o = part if init and at_key == lo else o + part
            at_key += m
            yield
        if last:
            abuf[mx, h, rows, :] = (o[:DH] / o[DH:DH + 1]).T.astype(BF16)
        else:
            mbuf[h, qc] = jnp.broadcast_to(new, (8, 256))
            acc[h, qc] = o

    def interleave(*streams):
        live = list(streams)
        while live:
            live = [s for s in live if next(s, live) is not live]

    def sweep(j, step, after=None, hooks=()):
        init, last = step == 0, step == 2
        spans = {0: ((2048, 256), (2048, 512)), 1: ((1024, 1024), (1024, 1024)), 2: ((0, 1024), (256, 768))}[step]
        bufs = ((s0, s1), (s2, s3)), ((t0, t1), (t2, t3))

        def make(g):
            return [scores(j * 4 + g, j, qc, *spans[qc], init, bufs[0][g % 2][qc], bufs[1][g % 2][qc])
                    for qc in range(2)]

        def use(g):
            return [weigh(j * 4 + g, j, qc, *spans[qc], init, last, bufs[0][g % 2][qc], bufs[1][g % 2][qc])
                    for qc in range(2)]

        interleave(*make(0))
        for g in range(4):
            interleave(*(make(g + 1) if g < 3 else []), *use(g))
            if after is not None:
                after(j * 4 + g)
            for when, steps in hooks:
                if when == g:
                    for name, *args in steps:
                        name(*args)

    def xcopy(kind, h, block, lo, n, to):
        ref = abuf.at[block, h, pl.ds(lo, n)]
        return pltpu.make_async_remote_copy(
            src_ref=ref, dst_ref=ref, send_sem=xs_sem.at[kind, h], recv_sem=xr_sem.at[kind, h],
            device_id=to, device_id_type=MESH)

    xl, xr, xo = (mx + 3) % 4, (mx + 1) % 4, (mx + 2) % 4

    def xsend(h):
        xcopy(0, h, mx, 0, TOK, xp).start()
        xcopy(1, h, mx, 0, TOK, xm).start()

    def xrelay(h):
        xcopy(0, h, xl, 0, TOK, xp).wait_recv()
        xcopy(2, h, xl, 0, 256, xp).start()
        xcopy(1, h, xr, 0, TOK, xm).wait_recv()
        xcopy(3, h, xr, 256, 256, xm).start()

    def xdone(h):
        xcopy(2, h, xo, 0, 256, xp).wait_recv()
        xcopy(3, h, xo, 256, 256, xm).wait_recv()

    parts = ((0, 512), (512, 512))

    def half(ref, i):
        return ref.at[pl.ds(*parts[i])]

    def wt(i, src, dst):
        return sm.remote(f"wt{i}", half(src, i), half(dst, i), swap)

    def wl(i):
        return pltpu.make_async_copy(half(w_ref, i), half(wbuf.at[c, y, z], i), loc_sem.at[12 + i])


    def w_hop(i, src):
        return sm.remote(f"wh{i}", half(src, i), half(wrelay, i), hop)

    def w_last(i, src):
        return sm.remote(f"wz{i}", half(src, i), half(wbuf.at[c, (mx + 2) % 4, z], i), ym)

    def w_swap(last):
        @pl.when(plus if last else off & jnp.logical_not(plus | far))
        def _():
            for i in range(2):
                wt(i, w_ref, wbuf.at[c, mx, z]).start()

        if not last:
            @pl.when(far)
            def _():
                for i in range(2):
                    w_hop(i, w_ref).start()

            @pl.when(jnp.logical_not(off))
            def _():
                for i in range(2):
                    wl(i).start()

    def w_passed(i):
        @pl.when(relays)
        def _():
            w_hop(i, wrelay).wait_recv()
            w_last(i, wrelay).start()

    def w_swapped(i):
        @pl.when(off & jnp.logical_not(far))
        def _():
            wt(i, wbuf.at[c, y, z], wbuf.at[c, y, z]).wait_recv()

        @pl.when(far)
        def _():
            w_last(i, wrelay).wait_recv()

        @pl.when(jnp.logical_not(off))
        def _():
            wl(i).wait()

    def w_side(d1, d2):
        b = wblock(d1, d2)
        sm.go(f"ws{d1}{d2}", b, b, sib)

    def w_send(d1, d2, second, halves=(0, 1), core=None):
        b = wblock(d1, d2)
        ds = []
        for i in halves:
            for sign, k in (("+", i), ("-", 1 - i if len(halves) == 2 else i)):
                ds.append(sm.remote(f"w{second}{sign}{d1}h{k}", half(b, k), half(b, k),
                                    along(not second, 1 if sign == "+" else -1)))
                if core in (None, 0):
                    sm.pending.append((f"w{second}{sign}{d1}h{k}", half(b, k).shape[0]))

        def start():
            for d in ds:
                d.start()

        if core is None:
            start()
        else:
            pl.when(c == core)(start)

    def w_got(sign, d1, second, i, b):
        sm.remote(f"w{second}{sign}{d1}h{i}", half(b, i), half(b, i), sib).wait_recv()

    def w_pair(d1, second):
        a, b = ((d1, -1), (d1, 1)) if second else ((-1, 0), (1, 0))
        return a, b

    def w_relay(d1, second):
        a, b = w_pair(d1, second)
        ra, rb = wblock(*a), wblock(*b)
        w_got("+", d1, second, 0, ra)
        sm.go(f"wr{second}+{d1}", half(ra, 0), half(ra, 0), along(not second, 1))
        w_got("-", d1, second, 1, rb)
        sm.go(f"wr{second}-{d1}", half(rb, 1), half(rb, 1), along(not second, -1))

    def w_rest(d1, second):
        a, b = w_pair(d1, second)
        w_got("+", d1, second, 1, wblock(*a))
        w_side(*a)
        w_got("-", d1, second, 0, wblock(*b))
        w_side(*b)

    def w_far(d1, second):
        o = (d1, 2) if second else (2, 0)
        b = wblock(*o)
        sm.remote(f"wr{second}+{d1}", half(b, 0), half(b, 0), sib).wait_recv()
        sm.remote(f"wr{second}-{d1}", half(b, 1), half(b, 1), sib).wait_recv()
        w_side(*o)

    def project_one(cc, terms, init, last=False):
        a = jnp.concatenate([abuf[x, j * 4 + g] for x, j in terms for g in range(4)], axis=1)
        for b in (0, 2):
            w = jnp.concatenate(
                [jnp.concatenate([wbuf[cc, x, b, pl.ds(j * 512, 512), :],
                                  wbuf[cc, x, b + 1, pl.ds(j * 512, 512), :]], axis=1)
                 for x, j in terms], axis=0)
            o = jnp.dot(a, w, preferred_element_type=F32)
            if not init:
                o = o + oacc[cc, b // 2]
            if last:
                for i in range(2):
                    cols = pl.ds(pl.multiple_of((2 * (b + i) + cc) * 128, 128), 128)
                    out_ref[:, cols] = o[:, i * 128:(i + 1) * 128].astype(BF16)
            else:
                oacc[cc, b // 2] = o

    def project(terms, init, last=False):
        @pl.loop(0, 2)
        def _(cc):
            project_one(cc, terms, init, last)

    kv_near(0)
    w_swap(False)
    for d in lq:
        d.wait()
    sweep(0, 0)
    sweep(1, 0)
    kv_mid(0)
    kv_fwd(0)
    kv_side(0)
    kv_near(1)
    w_swap(True)
    both_recv("d1", 0, 1)
    sweep(0, 1)
    w_passed(0)
    w_passed(1)
    kv_last(0)
    both_recv("d2", 0, 3)
    sweep(0, 2, xsend)
    kv_fwd(1)
    kv_mid(1)
    w_swapped(0)
    w_swapped(1)
    w_send(0, 0, 0)
    w_send(0, 0, 1, (0, 1), 0)
    kv_side(1)
    w_side(0, 0)
    both_recv("d1", 1, 1)
    sweep(1, 1, None, (
        (2, ((w_relay, 0, 0), (w_rest, 0, 0),
             (w_send, 1, 0, 1, (0, 1), 0), (w_send, -1, 0, 1, (0, 1), 0),
             (w_send, 0, 0, 1, (0, 1), 1), (w_send, 1, 0, 1, (0, 1), 1), (w_send, -1, 0, 1, (0, 1), 1))),
        (3, ((xrelay, 0),)),
    ))
    kv_last(1)
    both_recv("d2", 1, 3)
    sweep(1, 2, xsend, (
        (0, ((w_far, 0, 0), (w_send, 2, 0, 1))),
        (1, ((xrelay, 1),)),
        (3, ((xrelay, 2),)),
    ))
    w_relay(0, 1)
    w_relay(1, 1)
    xrelay(3)
    w_relay(-1, 1)
    xrelay(4)
    w_rest(0, 1)
    w_rest(1, 1)
    w_rest(-1, 1)
    w_far(0, 1)
    xrelay(5)
    w_relay(2, 1)
    w_far(1, 1)
    w_rest(2, 1)
    w_far(-1, 1)
    xrelay(6)
    w_far(2, 1)
    xrelay(7)
    for h in range(4):
        xdone(h)
    project_one(c, [(mx, 0), (mx, 1)], True)
    project_one(c, [(xl, 0), (xr, 0), (xo, 0)], False)
    for d1 in (0, -1, 1, 2):
        for d2 in (0, -1, 1, 2):
            sm.remote(f"ws{d1}{d2}", wbuf.at[1 - c, 0, 0], wbuf.at[1 - c, 0, 0], sib).wait_recv()
    project_one(1 - c, [(mx, 0), (mx, 1)], True)
    project_one(1 - c, [(xl, 0), (xr, 0), (xo, 0)], False)
    project([(xl, 1), (xr, 1)], False)
    for h in range(4, 8):
        xdone(h)
    project([(xo, 1)], False, True)

    for name, n in sm.pending:
        ref = wrelay.at[pl.ds(0, n)]
        sm.remote(name, ref, ref, sib).wait_send()
    for j in range(2):
        for kv in "kv":
            buf = kd if kv == "k" else vd
            r = slot(buf, j, 0)
            sm.remote(f"d1{kv}{j}", r, r, sib).wait_send()
            sm.remote(f"d2{kv}{j}", r, r, sib).wait_send()

    @pl.when(off)
    def _():
        @pl.when(jnp.logical_not(far))
        def _():
            for i in range(2):
                wt(i, w_ref, wbuf.at[c, mx, z]).wait_send()

    @pl.when(far)
    def _():
        for i in range(2):
            w_hop(i, w_ref).wait_send()

    @pl.when(relays)
    def _():
        for i in range(2):
            w_last(i, wrelay).wait_send()
    for h in range(8):
        xcopy(0, h, mx, 0, TOK, xp).wait_send()
        xcopy(1, h, mx, 0, TOK, xm).wait_send()
        xcopy(2, h, xl, 0, 256, xp).wait_send()
        xcopy(3, h, xr, 256, 256, xm).wait_send()


def body(queries, keys, values, doc_lengths, out_weight):
    hbm = pl.BlockSpec(memory_space=pl.ANY)
    vmem = pl.BlockSpec(memory_space=pltpu.VMEM)
    return pl.pallas_call(
        kernel,
        out_shape=pltpu.VMEM((TOK, 1024), BF16),
        in_specs=[hbm, hbm, hbm, hbm, vmem],
        out_specs=vmem,
        scratch_shapes=[
            pltpu.VMEM((8, TOK, DH), BF16),
            pltpu.VMEM((TOK, DH), BF16),
            pltpu.VMEM((2, ROWS, DH), BF16),
            pltpu.VMEM((ROWS, DH), BF16),
            pltpu.VMEM((2, TOK, DH), BF16),
            pltpu.VMEM((2, 5, DH, TOK), BF16),
            pltpu.VMEM((2, DH, TOK), BF16),
            pltpu.VMEM((1024, DH), BF16),
            pltpu.VMEM((2, 4, 4, 1024, DH), BF16),
            pltpu.VMEM((4, 8, TOK, DH), BF16),
            pltpu.VMEM((8, 2, 8, 256), F32),
            pltpu.VMEM((8, 2, DH + 16, 256), F32),
            *[pltpu.VMEM((1024, 256), F32)] * 4,
            *[pltpu.VMEM((8, 256), F32)] * 4,
            pltpu.VMEM((2, 2, TOK, 256), F32),
            pltpu.VMEM((8, DH), jnp.int32),
            pltpu.SemaphoreType.DMA((14,)),
            pltpu.SemaphoreType.DMA((96,)),
            pltpu.SemaphoreType.DMA((96,)),
            pltpu.SemaphoreType.DMA((4, 8)),
            pltpu.SemaphoreType.DMA((4, 8)),
        ],
        compiler_params=pltpu.CompilerParams(
            collective_id=0, has_side_effects=True, vmem_limit_bytes=60 * 1024 * 1024),
        name="attention_block",
    )(queries, keys, values, out_weight, doc_lengths.reshape(1, 64))


def solution(mesh):
    return jax.shard_map(
        body,
        mesh=mesh,
        in_specs=(P("seq", "head"), P("seq", "head"), P("seq", "head"), P(), P("head", "seq")),
        out_specs=P("seq", "head"),
        check_vma=False,
    )
```

```python
import jax
import jax.numpy as jnp
from jax import lax
from jax.experimental import pallas as pl
from jax.experimental.pallas import tpu as pltpu
from jax.sharding import PartitionSpec as P

DH = 128
TOK = 512
ROWS = 2560
FAR = 16384.0
LOG2E = 1.4426950408889634
C2 = LOG2E * DH ** -0.5
F32 = jnp.float32
BF16 = jnp.bfloat16
MESH = pl.DeviceIdType.MESH


class Sems:
    def __init__(self, send, recv):
        self.send, self.recv, self.names, self.pending = send, recv, {}, []

    def index(self, name):
        return self.names.setdefault(name, len(self.names))

    def remote(self, name, src, dst, dev):
        i = self.index(name)
        return pltpu.make_async_remote_copy(
            src_ref=src, dst_ref=dst, send_sem=self.send.at[i], recv_sem=self.recv.at[i],
            device_id=dev, device_id_type=MESH)

    def go(self, name, src, dst, dev):
        self.remote(name, src, dst, dev).start()
        self.pending.append((name, src.shape[0] * src.shape[1] // DH))


def kernel(q_ref, k_ref, v_ref, w_ref, len_ref, out_ref,
           qd, qcode, kd, kcode, vown, vd, vrelay, wrelay, wbuf, abuf, mbuf, acc, s0, s1, s2, s3, t0, t1, t2, t3, oacc, lens,
           loc_sem, send_sem, recv_sem, xs_sem, xr_sem):
    mx = lax.axis_index("head")
    s = lax.axis_index("seq")
    y = s // 8
    z = (s // 2) % 4
    c = s % 2
    sm = Sems(send_sem, recv_sem)

    def dev(seq, head=None):
        return {"seq": seq, "head": mx if head is None else head}

    def at(yy, zz, cc):
        return yy * 8 + zz * 2 + cc

    sib = dev(s + 1 - 2 * c)
    nxt = dev((s + 2) % 32)
    prv = dev((s + 30) % 32)
    zp, zm = dev(at(y, (z + 1) % 4, c)), dev(at(y, (z + 3) % 4, c))
    yp, ym = dev(at((y + 1) % 4, z, c)), dev(at((y + 3) % 4, z, c))
    xp, xm = dev(s, (mx + 1) % 4), dev(s, (mx + 3) % 4)
    p = y * 4 + z
    fwd = dev(((y * 4 + (z + 1) % 4 + 2) % 16) * 2 + c)
    po = (p + 14) % 16
    bwd = dev(at(po // 4, (po + 3) % 4, c))
    swap = {"seq": at(mx, z, c), "head": y}
    off = mx != y
    far, plus = (mx + 2) % 4 == y, mx == (y + 1) % 4
    hop, unhop = {"seq": at((y + 3) % 4, z, c), "head": y}, {"seq": at((y + 1) % 4, z, c), "head": (mx + 2) % 4}
    relays = plus
    f1, f2 = z + c * (y - z), y + c * (z - y)

    def along(first, step):
        d1, d2 = (step, 0) if first else (0, step)
        i1, i2 = (f1 + d1) % 4, (f2 + d2) % 4
        yy, zz = i2 + c * (i1 - i2), i1 + c * (i2 - i1)
        return dev(at(yy, zz, c))

    def wblock(d1, d2):
        i1, i2 = (f1 + d1) % 4, (f2 + d2) % 4
        yy, zz = i2 + c * (i1 - i2), i1 + c * (i2 - i1)
        return wbuf.at[c, yy, zz]

    loc = []

    def local(src, dst):
        d = pltpu.make_async_copy(src, dst, loc_sem.at[len(loc)])
        d.start()
        loc.append(d)
        return d

    own = pl.ds(2048, TOK)
    lk = [local(k_ref.at[:, pl.ds(j * DH, DH)], kd.at[j, own]) for j in range(2)]
    lv = [local(v_ref.at[:, pl.ds(j * DH, DH)], vown.at[j]) for j in range(2)]
    lq = [local(q_ref.at[:, pl.ds(h * DH, DH)], qd.at[h]) for h in range(8)]

    barrier = pltpu.get_barrier_semaphore()
    for peer in (sib, nxt, prv, zp, zm, yp, ym, xp, xm, fwd, bwd):
        pl.semaphore_signal(barrier, inc=1, device_id=peer, device_id_type=MESH)

    @pl.when(off & jnp.logical_not(far))
    def _():
        pl.semaphore_signal(barrier, inc=1, device_id=swap, device_id_type=MESH)

    @pl.when(far)
    def _():
        pl.semaphore_signal(barrier, inc=1, device_id=hop, device_id_type=MESH)

    @pl.when(relays)
    def _():
        pl.semaphore_signal(barrier, inc=1, device_id=unhop, device_id_type=MESH)

    lens[...] = jnp.zeros_like(lens)
    lens[0:1, 0:64] = len_ref[...]
    row = lens[0:1, :].astype(F32)
    i0 = lax.broadcasted_iota(jnp.int32, (DH, DH), 0)
    i1 = lax.broadcasted_iota(jnp.int32, (DH, DH), 1)
    col = jnp.sum(jnp.where(i1 < i0, jnp.broadcast_to(row, (DH, DH)), 0.0), axis=1, keepdims=True)
    start = jnp.sum(jnp.where(i0 == i1, jnp.broadcast_to(col, (DH, DH)), 0.0), axis=0, keepdims=True)
    end = start + row
    first = s * TOK

    @pl.loop(0, ROWS // 256)
    def _(b):
        pos = (first - 2048 + b * 256 + lax.broadcasted_iota(jnp.int32, (256, DH), 0)).astype(F32)
        inside = (pos >= start) & (pos < end)
        kcode[pl.ds(pl.multiple_of(b * 256, 256), 256), :] = jnp.where(inside, 0.0, -FAR).astype(BF16)

    for b in range(2):
        pos = (first + b * 256 + lax.broadcasted_iota(jnp.int32, (256, DH), 0)).astype(F32)
        inside = (pos >= start) & (pos < end)
        qcode[pl.ds(b * 256, 256), :] = jnp.where(inside, 1.0, 0.0).astype(BF16)

    for d in lk + lv:
        d.wait()
    for j in range(2):
        vd[j, 4] = vown[j].T
    pl.semaphore_wait(barrier, 11 + off.astype(jnp.int32) + relays.astype(jnp.int32))

    def slot(buf, j, i):
        if buf is vd:
            return vd.at[j, 4 - i]
        start_row = (4 - i) * TOK
        if not isinstance(i, int):
            start_row = pl.multiple_of(start_row, TOK)
        return buf.at[j, pl.ds(start_row, TOK)]

    def both(name, j, src, dst, to):
        sm.go(f"{name}k{j}", slot(kd, j, src), slot(kd, j, dst), to)
        sm.go(f"{name}v{j}", slot(vd, j, src), slot(vd, j, dst), to)

    def both_recv(name, j, dst):
        sm.remote(f"{name}k{j}", slot(kd, j, dst), slot(kd, j, dst), sib).wait_recv()
        sm.remote(f"{name}v{j}", slot(vd, j, dst), slot(vd, j, dst), sib).wait_recv()

    def side(name, j, src, dst, when):
        ds = [sm.remote(f"{name}k{j}", slot(kd, j, src), slot(kd, j, dst), sib),
              sm.remote(f"{name}v{j}", slot(vd, j, src), slot(vd, j, dst), sib)]

        @pl.when(when)
        def _():
            for d in ds:
                d.start()
        return ds

    def kv_near(j):
        sm.go(f"relay{j}", slot(vd, j, 0), vrelay.at[j], zm)
        both("near", j, 0, 2, nxt)
        side("d1", j, 0, 1, c == 0)

    def kv_fwd(j):
        sm.remote(f"relay{j}", vrelay.at[j], vrelay.at[j], sib).wait_recv()
        sm.go(f"farv{j}", vrelay.at[j], slot(vd, j, 4), fwd)

    def kv_mid(j):
        sm.remote(f"neark{j}", slot(kd, j, 2), slot(kd, j, 2), sib).wait_recv()
        sm.go(f"fark{j}", slot(kd, j, 2), slot(kd, j, 4), nxt)

    def kv_side(j):
        sm.remote(f"nearv{j}", slot(vd, j, 2), slot(vd, j, 2), sib).wait_recv()
        side("d1", j, 2, 1, c == 1)
        side("d2", j, 2, 3, c == 0)

    def kv_last(j):
        sm.remote(f"fark{j}", slot(kd, j, 4), slot(kd, j, 4), sib).wait_recv()
        sm.remote(f"farv{j}", slot(vd, j, 4), slot(vd, j, 4), sib).wait_recv()
        side("d2", j, 4, 3, c == 1)

    CK, WK = 1024, 256

    def scores(h, j, qc, lo, n, diag, sref, tref):
        rows = pl.ds(qc * 256, 256)
        qa = jnp.concatenate([qd[h, rows, :], qcode[rows, :]], axis=1)
        top = None
        for at_key in range(0, n, CK):
            m = min(CK, n - at_key)
            keys = pl.ds(lo + at_key, m)
            ka = jnp.concatenate([kd[j, keys, :], kcode[keys, :]], axis=1)
            sc = lax.dot_general(ka, qa, (((1,), (1,)), ((), ())), preferred_element_type=F32)
            if diag:
                u = at_key + lax.broadcasted_iota(jnp.int32, (m, 256), 0)
                r = lax.broadcasted_iota(jnp.int32, (m, 256), 1)
                sc = jnp.where(u <= r + qc * 256, sc, -FAR)
            sref[at_key:at_key + m, :] = sc
            best = jnp.max(sc.reshape(m // 8, 8, 256), axis=0)
            top = best if top is None else jnp.maximum(top, best)
            yield
        tref[...] = jnp.broadcast_to(jnp.max(top, axis=0, keepdims=True), (8, 256))

    def weigh(h, j, qc, lo, n, init, last, sref, tref):
        rows = pl.ds(qc * 256, 256)
        new = tref[0:1, :]
        if not init:
            old = mbuf[h, qc, 0:1, :]
            new = jnp.maximum(old, new)
            o = acc[h, qc] * jnp.exp2((old - new) * C2)
        at_key = lo
        while at_key < lo + n:
            m = min(WK, lo + n - at_key, TOK - at_key % TOK)
            pr = jnp.exp2((sref[pl.ds(at_key - lo, m), :] - new) * C2).astype(BF16)
            va = jnp.concatenate(
                [vd[j, at_key // TOK, :, pl.ds(at_key % TOK, m)], jnp.ones((16, m), BF16)], axis=0)
            part = jnp.dot(va, pr, preferred_element_type=F32)
            o = part if init and at_key == lo else o + part
            at_key += m
            yield
        if last:
            abuf[mx, h, rows, :] = (o[:DH] / o[DH:DH + 1]).T.astype(BF16)
        else:
            mbuf[h, qc] = jnp.broadcast_to(new, (8, 256))
            acc[h, qc] = o

    def interleave(*streams):
        live = list(streams)
        while live:
            live = [s for s in live if next(s, live) is not live]

    def sweep(j, step, after=None, hooks=()):
        init, last = step == 0, step == 2
        spans = {0: ((2048, 256), (2048, 512)), 1: ((1024, 1024), (1024, 1024)), 2: ((0, 1024), (256, 768))}[step]
        bufs = ((s0, s1), (s2, s3)), ((t0, t1), (t2, t3))

        def make(g):
            return [scores(j * 4 + g, j, qc, *spans[qc], init, bufs[0][g % 2][qc], bufs[1][g % 2][qc])
                    for qc in range(2)]

        def use(g):
            return [weigh(j * 4 + g, j, qc, *spans[qc], init, last, bufs[0][g % 2][qc], bufs[1][g % 2][qc])
                    for qc in range(2)]

        interleave(*make(0))
        for g in range(4):
            interleave(*(make(g + 1) if g < 3 else []), *use(g))
            if after is not None:
                after(j * 4 + g)
            for when, steps in hooks:
                if when == g:
                    for name, *args in steps:
                        name(*args)

    def xcopy(kind, h, block, lo, n, to):
        ref = abuf.at[block, h, pl.ds(lo, n)]
        return pltpu.make_async_remote_copy(
            src_ref=ref, dst_ref=ref, send_sem=xs_sem.at[kind, h], recv_sem=xr_sem.at[kind, h],
            device_id=to, device_id_type=MESH)

    xl, xr, xo = (mx + 3) % 4, (mx + 1) % 4, (mx + 2) % 4

    def xsend(h):
        xcopy(0, h, mx, 0, TOK, xp).start()
        xcopy(1, h, mx, 0, TOK, xm).start()

    def xrelay(h):
        xcopy(0, h, xl, 0, TOK, xp).wait_recv()
        xcopy(2, h, xl, 0, 256, xp).start()
        xcopy(1, h, xr, 0, TOK, xm).wait_recv()
        xcopy(3, h, xr, 256, 256, xm).start()

    def xdone(h):
        xcopy(2, h, xo, 0, 256, xp).wait_recv()
        xcopy(3, h, xo, 256, 256, xm).wait_recv()

    parts = ((0, 512), (512, 512))

    def half(ref, i):
        return ref.at[pl.ds(*parts[i])]

    def wt(i, src, dst):
        return sm.remote(f"wt{i}", half(src, i), half(dst, i), swap)

    def wl(i):
        return pltpu.make_async_copy(half(w_ref, i), half(wbuf.at[c, y, z], i), loc_sem.at[12 + i])


    def w_hop(i, src):
        return sm.remote(f"wh{i}", half(src, i), half(wrelay, i), hop)

    def w_last(i, src):
        return sm.remote(f"wz{i}", half(src, i), half(wbuf.at[c, (mx + 2) % 4, z], i), ym)

    def w_swap(last):
        @pl.when(plus if last else off & jnp.logical_not(plus | far))
        def _():
            for i in range(2):
                wt(i, w_ref, wbuf.at[c, mx, z]).start()

        if not last:
            @pl.when(far)
            def _():
                for i in range(2):
                    w_hop(i, w_ref).start()

            @pl.when(jnp.logical_not(off))
            def _():
                for i in range(2):
                    wl(i).start()

    def w_passed(i):
        @pl.when(relays)
        def _():
            w_hop(i, wrelay).wait_recv()
            w_last(i, wrelay).start()

    def w_swapped(i):
        @pl.when(off & jnp.logical_not(far))
        def _():
            wt(i, wbuf.at[c, y, z], wbuf.at[c, y, z]).wait_recv()

        @pl.when(far)
        def _():
            w_last(i, wrelay).wait_recv()

        @pl.when(jnp.logical_not(off))
        def _():
            wl(i).wait()

    def w_side(d1, d2):
        b = wblock(d1, d2)
        sm.go(f"ws{d1}{d2}", b, b, sib)

    def w_send(d1, d2, second, halves=(0, 1), core=None):
        b = wblock(d1, d2)
        ds = []
        for i in halves:
            for sign, k in (("+", i), ("-", 1 - i if len(halves) == 2 else i)):
                ds.append(sm.remote(f"w{second}{sign}{d1}h{k}", half(b, k), half(b, k),
                                    along(not second, 1 if sign == "+" else -1)))
                if core in (None, 0):
                    sm.pending.append((f"w{second}{sign}{d1}h{k}", half(b, k).shape[0]))

        def start():
            for d in ds:
                d.start()

        if core is None:
            start()
        else:
            pl.when(c == core)(start)

    def w_got(sign, d1, second, i, b):
        sm.remote(f"w{second}{sign}{d1}h{i}", half(b, i), half(b, i), sib).wait_recv()

    def w_pair(d1, second):
        a, b = ((d1, -1), (d1, 1)) if second else ((-1, 0), (1, 0))
        return a, b

    def w_relay(d1, second):
        a, b = w_pair(d1, second)
        ra, rb = wblock(*a), wblock(*b)
        w_got("+", d1, second, 0, ra)
        sm.go(f"wr{second}+{d1}", half(ra, 0), half(ra, 0), along(not second, 1))
        w_got("-", d1, second, 1, rb)
        sm.go(f"wr{second}-{d1}", half(rb, 1), half(rb, 1), along(not second, -1))

    def w_rest(d1, second):
        a, b = w_pair(d1, second)
        w_got("+", d1, second, 1, wblock(*a))
        w_side(*a)
        w_got("-", d1, second, 0, wblock(*b))
        w_side(*b)

    def w_far(d1, second):
        o = (d1, 2) if second else (2, 0)
        b = wblock(*o)
        sm.remote(f"wr{second}+{d1}", half(b, 0), half(b, 0), sib).wait_recv()
        sm.remote(f"wr{second}-{d1}", half(b, 1), half(b, 1), sib).wait_recv()
        w_side(*o)

    def project_one(cc, terms, init, last=False):
        a = jnp.concatenate([abuf[x, j * 4 + g] for x, j in terms for g in range(4)], axis=1)
        for b in (0, 2):
            w = jnp.concatenate(
                [jnp.concatenate([wbuf[cc, x, b, pl.ds(j * 512, 512), :],
                                  wbuf[cc, x, b + 1, pl.ds(j * 512, 512), :]], axis=1)
                 for x, j in terms], axis=0)
            o = jnp.dot(a, w, preferred_element_type=F32)
            if not init:
                o = o + oacc[cc, b // 2]
            if last:
                for i in range(2):
                    cols = pl.ds(pl.multiple_of((2 * (b + i) + cc) * 128, 128), 128)
                    out_ref[:, cols] = o[:, i * 128:(i + 1) * 128].astype(BF16)
            else:
                oacc[cc, b // 2] = o

    def project(terms, init, last=False):
        @pl.loop(0, 2)
        def _(cc):
            project_one(cc, terms, init, last)

    kv_near(0)
    w_swap(False)
    for d in lq:
        d.wait()
    sweep(0, 0)
    sweep(1, 0)
    kv_mid(0)
    kv_fwd(0)
    kv_side(0)
    kv_near(1)
    w_swap(True)
    both_recv("d1", 0, 1)
    sweep(0, 1)
    w_passed(0)
    w_passed(1)
    kv_last(0)
    both_recv("d2", 0, 3)
    sweep(0, 2, xsend)
    kv_fwd(1)
    kv_mid(1)
    w_swapped(0)
    w_swapped(1)
    w_send(0, 0, 0)
    w_send(0, 0, 1, (0, 1), 0)
    kv_side(1)
    w_side(0, 0)
    both_recv("d1", 1, 1)
    sweep(1, 1, None, (
        (2, ((w_relay, 0, 0), (w_rest, 0, 0),
             (w_send, 1, 0, 1, (0, 1), 0), (w_send, -1, 0, 1, (0, 1), 0),
             (w_send, 0, 0, 1, (0, 1), 1), (w_send, 1, 0, 1, (0, 1), 1), (w_send, -1, 0, 1, (0, 1), 1))),
        (3, ((xrelay, 0),)),
    ))
    xrelay(1)
    kv_last(1)
    both_recv("d2", 1, 3)
    sweep(1, 2, xsend, (
        (0, ((w_far, 0, 0), (w_send, 2, 0, 1))),
        (1, ((xrelay, 2),)),
    ))
    w_relay(0, 1)
    w_relay(1, 1)
    xrelay(3)
    w_relay(-1, 1)
    xrelay(4)
    w_relay(2, 1)
    w_rest(0, 1)
    w_rest(1, 1)
    w_rest(-1, 1)
    xrelay(5)
    w_far(0, 1)
    w_far(1, 1)
    w_rest(2, 1)
    xrelay(6)
    w_far(-1, 1)
    xrelay(7)
    w_far(2, 1)
    for h in range(4):
        xdone(h)
    project_one(c, [(mx, 0), (mx, 1)], True)
    project_one(c, [(xl, 0), (xr, 0), (xo, 0)], False)
    for d1 in (0, -1, 1, 2):
        for d2 in (0, -1, 1, 2):
            sm.remote(f"ws{d1}{d2}", wbuf.at[1 - c, 0, 0], wbuf.at[1 - c, 0, 0], sib).wait_recv()
    project_one(1 - c, [(mx, 0), (mx, 1)], True)
    project_one(1 - c, [(xl, 0), (xr, 0), (xo, 0)], False)
    project([(xl, 1), (xr, 1)], False)
    for h in range(4, 8):
        xdone(h)
    project([(xo, 1)], False, True)

    for name, n in sm.pending:
        ref = wrelay.at[pl.ds(0, n)]
        sm.remote(name, ref, ref, sib).wait_send()
    for j in range(2):
        for kv in "kv":
            buf = kd if kv == "k" else vd
            r = slot(buf, j, 0)
            sm.remote(f"d1{kv}{j}", r, r, sib).wait_send()
            sm.remote(f"d2{kv}{j}", r, r, sib).wait_send()

    @pl.when(off)
    def _():
        @pl.when(jnp.logical_not(far))
        def _():
            for i in range(2):
                wt(i, w_ref, wbuf.at[c, mx, z]).wait_send()

    @pl.when(far)
    def _():
        for i in range(2):
            w_hop(i, w_ref).wait_send()

    @pl.when(relays)
    def _():
        for i in range(2):
            w_last(i, wrelay).wait_send()
    for h in range(8):
        xcopy(0, h, mx, 0, TOK, xp).wait_send()
        xcopy(1, h, mx, 0, TOK, xm).wait_send()
        xcopy(2, h, xl, 0, 256, xp).wait_send()
        xcopy(3, h, xr, 256, 256, xm).wait_send()


def body(queries, keys, values, doc_lengths, out_weight):
    hbm = pl.BlockSpec(memory_space=pl.ANY)
    vmem = pl.BlockSpec(memory_space=pltpu.VMEM)
    return pl.pallas_call(
        kernel,
        out_shape=pltpu.VMEM((TOK, 1024), BF16),
        in_specs=[hbm, hbm, hbm, hbm, vmem],
        out_specs=vmem,
        scratch_shapes=[
            pltpu.VMEM((8, TOK, DH), BF16),
            pltpu.VMEM((TOK, DH), BF16),
            pltpu.VMEM((2, ROWS, DH), BF16),
            pltpu.VMEM((ROWS, DH), BF16),
            pltpu.VMEM((2, TOK, DH), BF16),
            pltpu.VMEM((2, 5, DH, TOK), BF16),
            pltpu.VMEM((2, DH, TOK), BF16),
            pltpu.VMEM((1024, DH), BF16),
            pltpu.VMEM((2, 4, 4, 1024, DH), BF16),
            pltpu.VMEM((4, 8, TOK, DH), BF16),
            pltpu.VMEM((8, 2, 8, 256), F32),
            pltpu.VMEM((8, 2, DH + 16, 256), F32),
            *[pltpu.VMEM((1024, 256), F32)] * 4,
            *[pltpu.VMEM((8, 256), F32)] * 4,
            pltpu.VMEM((2, 2, TOK, 256), F32),
            pltpu.VMEM((8, DH), jnp.int32),
            pltpu.SemaphoreType.DMA((14,)),
            pltpu.SemaphoreType.DMA((96,)),
            pltpu.SemaphoreType.DMA((96,)),
            pltpu.SemaphoreType.DMA((4, 8)),
            pltpu.SemaphoreType.DMA((4, 8)),
        ],
        compiler_params=pltpu.CompilerParams(
            collective_id=0, has_side_effects=True, vmem_limit_bytes=60 * 1024 * 1024),
        name="attention_block",
    )(queries, keys, values, out_weight, doc_lengths.reshape(1, 64))


def solution(mesh):
    return jax.shard_map(
        body,
        mesh=mesh,
        in_specs=(P("seq", "head"), P("seq", "head"), P("seq", "head"), P(), P("head", "seq")),
        out_specs=P("seq", "head"),
        check_vma=False,
    )
```
